32 devices in a mesh: patch: 8 (over z, y), sub: 4 (over x, core).
Axes of the slice: x: 2, y: 2, z: 4, core: 2. Of those that a mesh axis runs over, the one named last changes fastest.
Arguments:
- state: float32 [8, 4, 1, 27, 729], P('patch', 'sub'), may hold values from -6 to 6
- stiff_weight: float32 [8, 96, 9216], P('patch'), may hold values from 0.3 to 3
- volume_weight: float32 [8, 96, 9216], P('patch'), may hold values from 0.5 to 2
- lagrange: float32 [32, 4, 1, 729], P('patch', 'sub'), may hold values from -6 to 6
- mortar: float32 [32, 2, 2, 27, 27], P('patch'), may hold values from -1.25 to 1.25
- links: int32 [32, 6], replicated, may hold values from 0 to 27, as said below
Outputs:
- residual: float32 [8, 4, 1, 27, 729], P('patch', 'sub')
- constraint: float32 [32, 4, 1, 729], P('patch', 'sub')
The draws below stay inside these ranges and needn't reach their ends.
Inputs may be any that keep to these rules, and one draw needn't show every extreme that they name: `links`: row o * 4 + s is slot s of owner o along patch. Live slots of an owner come first and have both counts in 12 to 27; empty slots are all zero. 2 * 8 slots are live. A live interface joins face 2d + 1 of its first patch to face 2d of its second patch, d being 0 or 1; faces 0 to 3 of every patch lie on exactly one live interface each; the live interfaces of one owner all have the same d. At most 2 faces of one patch lie on live interfaces of one owner; in every draw some owner has 4 live slots and 2 faces of one patch.
All inputs are finite; a program needn't handle non-finite values.
Results may differ from the reference program's by a relative error of at most 0.0001.
Values sent between devices are 32-bit elements; how exact they have to be, the bound alone decides.
No kernel may reach another device: no remote copies, remote signals or barrier semaphores. Data moves between devices by JAX's collectives and lax.ppermute only.
A program may use at most 128 MiB of HBM per device.

```python
import math
import jax
import jax.numpy as jnp
import numpy as np
from jax import lax

ELEMS = 24
DEGREE = 3
FIELDS = 4
VECS = 1
SLOTS = 4
BASIS = 27
QUAD = 96
QLO = 12
PATCHES = 8


def draw_links(key, part):
    count = PATCHES
    streams = jax.random.split(jax.random.fold_in(key, 17), 5)
    cycles = jnp.stack([jax.random.permutation(streams[0], count), jax.random.permutation(streams[1], count)])
    owner_order = jax.random.permutation(streams[2], count)
    shifts = jax.random.randint(streams[3], (count // 2,), -2, 3).at[0].set(2)
    pair_loads = jnp.stack([2 + shifts, 2 - shifts], axis=1).reshape(count)
    order_starts = jnp.cumsum(pair_loads) - pair_loads
    position = jnp.argsort(owner_order)
    loads = pair_loads[position]
    starts = order_starts[position]
    slot_ids = jnp.arange(SLOTS)
    edges = starts[:, None] + slot_ids[None, :]
    alive = (slot_ids[None, :] < loads[:, None]).astype(jnp.int32)
    direction = jnp.minimum(edges // count, 1)
    along = edges % count
    first_patch = cycles[direction, along]
    second_patch = cycles[direction, (along + 1) % count]
    extents = jax.random.randint(streams[4], (count, SLOTS, 2), QLO, BASIS + 1)
    table = jnp.stack([first_patch, second_patch, 2 * direction + 1, 2 * direction, extents[:, :, 0], extents[:, :, 1]], axis=-1)
    return (table * alive[:, :, None]).reshape(count * SLOTS, 6).astype(jnp.int32)


def block_levels(key, extent, shards, smallest, largest):
    level = 1.0
    for dim, parts in shards:
        steps = jax.random.uniform(jax.random.fold_in(jax.random.fold_in(key, 6), dim), (parts,), jnp.float32, smallest / len(shards), largest / len(shards))
        level = level * jnp.repeat(jnp.exp(steps), extent[dim] // parts).reshape((-1,) + (1,) * (len(extent) - 1 - dim))
    return level


def bell_draw(stream_key, extent, width, most, cuts=(), dtype=jnp.bfloat16):
    values = jax.random.normal(stream_key, extent, jnp.float32) * width
    if len(cuts) > 0:
        values = block_levels(stream_key, extent, cuts, -0.22, 0.18) * values
    return jnp.clip(values, min=-most, max=most).astype(dtype)


def setup_inputs(seed: int = 0) -> dict:
    splits = jax.random.split(jax.random.key(seed), 7)
    return {
        "state": bell_draw(splits[0], (PATCHES, FIELDS, VECS, BASIS, BASIS * BASIS), 1.0, 6.0, ((0, 8), (1, 4)), jnp.float32),
        "stiff_weight": jnp.clip(jnp.exp(math.log(3.0) - 2.3025851 * jax.random.uniform(splits[1], (PATCHES, QUAD, QUAD * QUAD), jnp.float32) ** block_levels(splits[1], (PATCHES, QUAD, QUAD * QUAD), ((0, 8),), -0.2, 0.2)), 0.3, 3.0),
        "volume_weight": jnp.clip(jnp.exp(math.log(2.0) - 1.3862944 * jax.random.uniform(splits[2], (PATCHES, QUAD, QUAD * QUAD), jnp.float32) ** block_levels(splits[2], (PATCHES, QUAD, QUAD * QUAD), ((0, 8),), -0.2, 0.2)), 0.5, 2.0),
        "lagrange": bell_draw(splits[3], (PATCHES * SLOTS, FIELDS, VECS, BASIS * BASIS), 1.0, 6.0, ((0, 8), (1, 4)), jnp.float32),
        "mortar": bell_draw(splits[4], (PATCHES * SLOTS, 2, 2, BASIS, BASIS), BASIS ** -0.5, 1.25, ((0, 8),), jnp.float32),
        "links": draw_links(jax.random.fold_in(splits[6], 71), 0),
    }


stabilize = 0.25
highest = lax.Precision.HIGHEST
gauss_points_four = [-0.8611363115940526, -0.3399810435848563, 0.3399810435848563, 0.8611363115940526]
gauss_weights_four = [0.3478548451374538, 0.6521451548625461, 0.6521451548625461, 0.3478548451374538]


def spline_tables(elements, degree):
    knot_list = np.concatenate([np.zeros(degree), np.arange(elements + 1.0), np.full(degree, float(elements))])
    gauss_nodes = np.array(gauss_points_four)
    gauss_weights = np.array(gauss_weights_four)
    points = (np.arange(elements)[:, None] + (gauss_nodes[None, :] + 1.0) / 2.0).reshape(-1)
    point_weights = np.tile(gauss_weights / 2.0, elements)
    current = np.where((knot_list[None, :-1] <= points[:, None]) & (points[:, None] < knot_list[None, 1:]), 1.0, 0.0)
    previous = current
    for order_k in range(1, degree + 1):
        previous = current
        amount = len(knot_list) - 1 - order_k
        current = np.zeros((points.shape[0], amount))
        for column in range(amount):
            left_span = knot_list[column + order_k] - knot_list[column]
            right_span = knot_list[column + order_k + 1] - knot_list[column + 1]
            if left_span > 0:
                current[:, column] += (points - knot_list[column]) / left_span * previous[:, column]
            if right_span > 0:
                current[:, column] += (knot_list[column + order_k + 1] - points) / right_span * previous[:, column + 1]
    slope_part = np.zeros(current.shape)
    for column in range(current.shape[1]):
        left_span = knot_list[column + degree] - knot_list[column]
        right_span = knot_list[column + degree + 1] - knot_list[column + 1]
        if left_span > 0:
            slope_part[:, column] += degree / left_span * previous[:, column]
        if right_span > 0:
            slope_part[:, column] -= degree / right_span * previous[:, column + 1]
    return (jnp.asarray(current, jnp.float32), jnp.asarray(slope_part, jnp.float32),
            jnp.asarray(current * point_weights[:, None], jnp.float32),
            jnp.asarray(slope_part * point_weights[:, None], jnp.float32))


def forward(coefficients, outer_matrix, middle_matrix, inner_matrix):
    size_n = outer_matrix.shape[1]
    partial_value = coefficients.reshape(size_n, size_n, size_n)
    partial_value = jnp.einsum('ck,ijk->ijc', inner_matrix, partial_value, precision=highest)
    partial_value = jnp.einsum('bj,ijc->ibc', middle_matrix, partial_value, precision=highest)
    return jnp.dot(outer_matrix, partial_value.reshape(size_n, -1), precision=highest, preferred_element_type=jnp.float32)


def backward(values, outer_matrix, middle_matrix, inner_matrix):
    size_n = outer_matrix.shape[1]
    points = outer_matrix.shape[0]
    partial_value = jnp.dot(outer_matrix.T, values, precision=highest, preferred_element_type=jnp.float32)
    partial_value = partial_value.reshape(size_n, points, points)
    partial_value = jnp.einsum('bj,ibc->ijc', middle_matrix, partial_value, precision=highest)
    partial_value = jnp.einsum('ck,ijc->ijk', inner_matrix, partial_value, precision=highest)
    return partial_value.reshape(size_n, size_n * size_n)


def reference(state, stiff_weight, volume_weight, lagrange, mortar, links):
    value_table, slope_table, value_weighted, slope_weighted = spline_tables(ELEMS, DEGREE)
    size_n = BASIS
    slopes = [(slope_table, value_table, value_table), (value_table, slope_table, value_table),
              (value_table, value_table, slope_table)]
    weighted = [(slope_weighted, value_weighted, value_weighted), (value_weighted, slope_weighted, value_weighted),
                (value_weighted, value_weighted, slope_weighted)]

    def one_patch(packed):
        fields, stiffness, volume = packed

        def one_vector(group):
            pvalue = forward(group[3], value_table, value_table, value_table)
            outputs = []
            for comp in range(3):
                total = jnp.zeros((size_n, size_n * size_n), jnp.float32)
                for axis_d in range(3):
                    flux = stiffness * forward(group[comp], slopes[axis_d][0], slopes[axis_d][1], slopes[axis_d][2])
                    if axis_d == comp:
                        flux = flux - volume * pvalue
                    total = total + backward(flux, weighted[axis_d][0], weighted[axis_d][1], weighted[axis_d][2])
                outputs.append(total)
            pressure_total = jnp.zeros((size_n, size_n * size_n), jnp.float32)
            for axis_d in range(3):
                flux = -stabilize * stiffness * forward(group[3], slopes[axis_d][0], slopes[axis_d][1], slopes[axis_d][2])
                pressure_total = pressure_total + backward(flux, weighted[axis_d][0], weighted[axis_d][1], weighted[axis_d][2])
            for comp in range(3):
                flux = volume * forward(group[comp], slopes[comp][0], slopes[comp][1], slopes[comp][2])
                pressure_total = pressure_total - backward(flux, value_weighted, value_weighted, value_weighted)
            outputs.append(pressure_total)
            return jnp.stack(outputs)

        return jnp.moveaxis(lax.map(one_vector, jnp.moveaxis(fields, 1, 0)), 0, 1)

    volume_part = lax.map(one_patch, (state, stiff_weight, volume_weight))
    patches = state.shape[0]
    vectors = state.shape[2]
    cube = state.reshape(patches, FIELDS, vectors, size_n, size_n, size_n)
    faces = jnp.stack([cube[:, :, :, 0], cube[:, :, :, -1], cube[:, :, :, :, 0], cube[:, :, :, :, -1]], axis=1)
    item_patch = links[:, 0:2]
    item_face = links[:, 2:4]
    item_traces = faces[item_patch, item_face]
    rank_grid = jnp.arange(size_n).astype(jnp.int32)
    row_mask = (rank_grid[None, :] < links[:, 4:5]).astype(jnp.float32)
    col_mask = (rank_grid[None, :] < links[:, 5:6]).astype(jnp.float32)
    left = mortar[:, :, 0] * row_mask[:, None, :, None]
    right = mortar[:, :, 1] * col_mask[:, None, :, None]
    projected = jnp.einsum('rsai,rsfvij,rsbj->rsfvab', left, item_traces, right, precision=highest)
    link_rows = links.shape[0]
    constraint = (projected[:, 0] - projected[:, 1]).reshape(link_rows, FIELDS, vectors, size_n * size_n)
    multipliers = lagrange.reshape(link_rows, FIELDS, vectors, size_n, size_n)
    signs = jnp.array([1.0, -1.0], jnp.float32)
    correction = jnp.einsum('rsai,rfvab,rsbj->rsfvij', left, multipliers, right, precision=highest)
    correction = correction * signs[None, :, None, None, None, None]
    segment_ids = (item_patch * 4 + item_face).reshape(-1).astype(jnp.int32)
    face_total = jax.ops.segment_sum(correction.reshape(link_rows * 2, FIELDS, vectors, size_n, size_n),
                                     segment_ids, num_segments=patches * 4)
    face_total = face_total.reshape(patches, 4, FIELDS, vectors, size_n, size_n)
    result = volume_part.reshape(patches, FIELDS, vectors, size_n, size_n, size_n)
    result = result.at[:, :, :, 0].add(face_total[:, 0])
    result = result.at[:, :, :, -1].add(face_total[:, 1])
    result = result.at[:, :, :, :, 0].add(face_total[:, 2])
    result = result.at[:, :, :, :, -1].add(face_total[:, 3])
    return result.reshape(patches, FIELDS, vectors, size_n, size_n * size_n), constraint
```

```python
import functools

import jax
import jax.numpy as jnp
import numpy as np
from jax import lax
from jax.experimental import pallas as pl
from jax.experimental.pallas import tpu as pltpu
from jax.sharding import PartitionSpec as P

ELEMS = 24
DEGREE = 3
FIELDS = 4
LOCAL = DEGREE + 1
NODES = 4
BASIS = ELEMS + DEGREE
QUAD = ELEMS * NODES
PAD = 32
WIN = LOCAL * PAD
SPAN = NODES * QUAD
GROUPS = ELEMS // 4
WIDE = (GROUPS + 1) * WIN
FLAT = 768

stabilize = 0.25
highest = lax.Precision.HIGHEST
f32 = jnp.float32
bf16 = jnp.bfloat16
gauss_points_four = [
    -0.8611363115940526,
    -0.3399810435848563,
    0.3399810435848563,
    0.8611363115940526,
]
gauss_weights_four = [
    0.3478548451374538,
    0.6521451548625461,
    0.6521451548625461,
    0.3478548451374538,
]


def spline_tables(knot_list, points, degree):
    current = np.where(
        (knot_list[None, :-1] <= points[:, None]) & (points[:, None] < knot_list[None, 1:]),
        1.0,
        0.0,
    )
    previous = current
    for order_k in range(1, degree + 1):
        previous = current
        amount = len(knot_list) - 1 - order_k
        current = np.zeros((points.shape[0], amount))
        for column in range(amount):
            left_span = knot_list[column + order_k] - knot_list[column]
            right_span = knot_list[column + order_k + 1] - knot_list[column + 1]
            if left_span > 0:
                current[:, column] += (points - knot_list[column]) / left_span * previous[:, column]
            if right_span > 0:
                current[:, column] += (
                    (knot_list[column + order_k + 1] - points)
                    / right_span
                    * previous[:, column + 1]
                )
    slope_part = np.zeros(current.shape)
    for column in range(current.shape[1]):
        left_span = knot_list[column + degree] - knot_list[column]
        right_span = knot_list[column + degree + 1] - knot_list[column + 1]
        if left_span > 0:
            slope_part[:, column] += degree / left_span * previous[:, column]
        if right_span > 0:
            slope_part[:, column] -= degree / right_span * previous[:, column + 1]
    return current, slope_part


def halves(table):
    high = table.astype(np.dtype(bf16)).astype(np.float64)
    return high, table - high


def padded(table, rows, cols):
    out = np.zeros((rows, cols))
    out[: table.shape[0], : table.shape[1]] = table
    return out


@functools.cache
def constants():
    nodes = np.array(gauss_points_four)
    points = (np.arange(ELEMS)[:, None] + (nodes[None, :] + 1.0) / 2.0).reshape(-1)
    weights = np.tile(np.array(gauss_weights_four) / 2.0, ELEMS)
    open_knots = np.concatenate(
        [np.zeros(DEGREE), np.arange(ELEMS + 1.0), np.full(DEGREE, float(ELEMS))]
    )
    even_knots = np.arange(-DEGREE, ELEMS + DEGREE + 1.0)
    value, slope = spline_tables(open_knots, points, DEGREE)
    even_value, even_slope = spline_tables(even_knots, points, DEGREE)
    change = np.round(np.linalg.lstsq(even_value, value, rcond=None)[0] * 4.0) / 4.0
    local_value = even_value[4 * NODES : 5 * NODES, 4 : 4 + LOCAL]
    local_slope = even_slope[4 * NODES : 5 * NODES, 4 : 4 + LOCAL]
    local_w = weights[:NODES, None]

    def kron(local, table):
        wide = padded(table, QUAD, PAD)
        return np.einsum("bj,ck->jkbc", local, wide).reshape(WIN, SPAN)

    ahead = np.concatenate(
        [kron(local_value, value), kron(local_slope, value), kron(local_value, slope)], axis=1
    )
    value_w, slope_w = value * weights[:, None], slope * weights[:, None]
    back = np.concatenate(
        [
            kron(local_value * local_w, value_w).T,
            kron(local_slope * local_w, value_w).T,
            kron(local_value * local_w, slope_w).T,
            ],
        axis=0,
    )
    ahead_high, ahead_low = halves(ahead)
    ahead3 = np.concatenate([ahead_high, ahead_high, ahead_low], axis=0)
    back_high, back_low = halves(back)
    back2 = np.concatenate([back_high, back_low], axis=1)

    def left3(table):
        high, low = halves(padded(table, QUAD, PAD))
        return np.concatenate([high, high, low], axis=1)

    def left4(table):
        high, low = halves(padded(table, QUAD, PAD).T)
        return np.concatenate(
            [np.concatenate([high, high], axis=1), np.concatenate([low, low], axis=1)], axis=0
        )

    spread = np.zeros((BASIS, BASIS, WIDE // PAD, PAD))
    for k in range(BASIS):
        spread[:, k, :BASIS, k] = change.T
    spread = padded(spread.reshape(BASIS * BASIS, WIDE), FLAT, WIDE)
    fold = np.zeros((FLAT, PAD))
    for j in range(BASIS):
        fold[j * BASIS : (j + 1) * BASIS, :BASIS] = np.eye(BASIS)
    group = np.full((8, FLAT), 99, np.int32)
    group[:, : BASIS * BASIS] = np.arange(BASIS * BASIS)[None, :] // BASIS
    as16 = lambda a: a.astype(np.dtype(bf16))
    return dict(
        ahead=as16(ahead3),
        back=as16(back2),
        outer=as16(np.stack([left3(slope), left3(value)])),
        inner=as16(np.stack([left4(slope_w), left4(value_w)])),
        spread=as16(spread),
        fold=as16(fold),
        group=group,
    )


def split(x):
    high = x.astype(bf16)
    return high, (x - high.astype(f32)).astype(bf16)


def dot(a, b):
    return jnp.dot(a, b, preferred_element_type=f32)


def dot_nt(a, b):
    return lax.dot_general(a, b, (((1,), (1,)), ((), ())), preferred_element_type=f32)


def expand(fields, spread):
    count = len(fields)
    parts = []
    for field in fields:
        parts.extend(split(field))
    out = dot(jnp.concatenate(parts, axis=0), spread)
    return [out[2 * n * PAD : (2 * n + 1) * PAD] + out[(2 * n + 1) * PAD : (2 * n + 2) * PAD] for n in range(count)]


def windows(wide, groups):
    shifted = [wide] + [pltpu.roll(wide, WIDE - PAD * r, axis=1) for r in range(1, 4)]
    shifted = [split(x) for x in shifted]
    rows = []
    for m in groups:
        for r in range(4):
            high = shifted[r][0][:, m * WIN : (m + 1) * WIN]
            low = shifted[r][1][:, m * WIN : (m + 1) * WIN]
            rows.append(jnp.concatenate([high, low, high], axis=1))
    return jnp.concatenate(rows, axis=0)


def overlap(rows, groups):
    first, count = groups[0], len(groups)
    total = None
    for r in range(4):
        pieces = []
        if first > 0:
            pieces.append(jnp.zeros((PAD, first * WIN), f32))
        pieces.extend(rows[(4 * n + r) * PAD : (4 * n + r + 1) * PAD] for n in range(count))
        rest = WIDE // WIN - first - count
        pieces.append(jnp.zeros((PAD, rest * WIN), f32))
        line = jnp.concatenate(pieces, axis=1)
        if r > 0:
            line = pltpu.roll(line, PAD * r, axis=1)
        total = line if total is None else total + line
    return total


def gather_back(heads, back, count):
    out = dot(heads, back)
    rows = count * PAD
    out = out[:rows] + out[rows:]
    return out[:, :WIN] + out[:, WIN:]


def load_flat(dst, src):
    dst[...] = jnp.zeros(dst.shape, f32)
    dst[:BASIS, : BASIS * BASIS] = src


def stiff_kernel(groups, expand_here, field_ref, spread_ref, ahead_ref, outer_ref, inner_ref, back_ref, weight_hbm, *rest):
    if expand_here:
        out_ref, wide_ref, flat, weight, mid_h, mid_l, heads, sems = rest
    else:
        out_ref, weight, mid_h, mid_l, heads, sems = rest
    step = 4 * SPAN
    copies = [
        pltpu.make_async_copy(
            weight_hbm.at[0, :, pl.ds(m * step, step)], weight.at[:, pl.ds(n * step, step)], sems.at[n]
        )
        for n, m in enumerate(groups)
    ]
    for copy in copies:
        copy.start()
    if expand_here:
        load_flat(flat, field_ref[0, 0, 0])
        (wide,) = expand([flat[...]], spread_ref[...])
        wide_ref[...] = wide
    else:
        wide = field_ref[...]
    lhs = windows(wide, groups)
    count = 4 * len(groups)
    rows = count * PAD
    mid = dot(lhs, ahead_ref[...])
    high, low = split(mid)
    mid_h[...] = high
    mid_l[...] = low
    for n in range(len(groups)):
        copies[n].wait()
        for r in range(4):
            e = 4 * n + r
            at = slice(e * PAD, (e + 1) * PAD)
            stack = jnp.concatenate([mid_h[at, :], mid_l[at, :], mid_h[at, :]], axis=0)
            first = dot(outer_ref[0], stack[:, :SPAN])
            others = dot(outer_ref[1], stack[:, SPAN:])
            scale = weight[:, e * SPAN : (e + 1) * SPAN]
            first = first * scale
            others = others * jnp.concatenate([scale, scale], axis=1)
            first = dot(inner_ref[0], jnp.concatenate(split(first), axis=0))
            others = dot(inner_ref[1], jnp.concatenate(split(others), axis=0))
            high, low = split(first[:PAD] + first[PAD:])
            heads[at, :SPAN] = high
            heads[rows + e * PAD : rows + (e + 1) * PAD, :SPAN] = low
            high, low = split(others[:PAD] + others[PAD:])
            heads[at, SPAN:] = high
            heads[rows + e * PAD : rows + (e + 1) * PAD, SPAN:] = low
    out_ref[...] = overlap(gather_back(heads[...], back_ref[...], count), groups)


def volume_kernel(place_ref, near_ref, far_ref, spread_ref, ahead_ref, outer_ref, inner_ref, back_ref, weight_hbm, out_ref, flat, weight, mid_h, mid_l, heads, sems):
    groups = list(range(GROUPS))
    step = 4 * SPAN
    copies = [
        pltpu.make_async_copy(
            weight_hbm.at[0, :, pl.ds(m * step, step)], weight.at[:, pl.ds(m * step, step)], sems.at[m]
        )
        for m in groups
    ]
    for copy in copies:
        copy.start()
    sub = place_ref[1]
    is_pressure = sub == FIELDS - 1
    load_flat(flat.at[0], near_ref[0, 0, 0])
    load_flat(flat.at[1], far_ref[0])
    load_flat(flat.at[2], far_ref[1])
    chosen = jnp.where(is_pressure, 2, 2 - sub)
    zero = jnp.zeros((PAD, FLAT), f32)
    fields = [
        flat[chosen],
        jnp.where(is_pressure, flat[1], zero),
        jnp.where(is_pressure, flat[0], zero),
    ]
    wides = expand(fields, spread_ref[...])
    count = 4 * len(groups)
    rows = count * PAD
    mid = dot(windows(wides[0], groups), ahead_ref[:, :SPAN])
    high, low = split(mid)
    mid_h[:, :SPAN] = high
    mid_l[:, :SPAN] = low
    mid = dot(windows(wides[1], groups), ahead_ref[:, SPAN : 2 * SPAN]) + dot(
        windows(wides[2], groups), ahead_ref[:, 2 * SPAN :]
    )
    high, low = split(mid)
    mid_h[:, SPAN:] = high
    mid_l[:, SPAN:] = low
    along = jnp.where(is_pressure, 0, 1)
    outer = jnp.concatenate([outer_ref[along], outer_ref[1]], axis=1)
    inner = inner_ref[jnp.where(sub == 0, 0, 1)]
    for n in range(len(groups)):
        copies[n].wait()
        for r in range(4):
            e = 4 * n + r
            at = slice(e * PAD, (e + 1) * PAD)
            stack = jnp.concatenate(
                [mid_h[at, :SPAN], mid_l[at, :SPAN], mid_h[at, :SPAN], mid_h[at, SPAN:], mid_l[at, SPAN:], mid_h[at, SPAN:]],
                axis=0,
            )
            value = dot(outer, stack) * weight[:, e * SPAN : (e + 1) * SPAN]
            value = dot(inner, jnp.concatenate(split(value), axis=0))
            high, low = split(value[:PAD] + value[PAD:])
            heads[at, :] = high
            heads[rows + e * PAD : rows + (e + 1) * PAD, :] = low
    kind = jnp.where(is_pressure, 0, sub)
    back = back_ref[pl.ds(pl.multiple_of(kind * SPAN, SPAN), SPAN), :]
    out_ref[...] = overlap(gather_back(heads[...], back, count), groups)


def masked(matrix, limit):
    rows = lax.broadcasted_iota(jnp.int32, matrix.shape, 0)
    return jnp.where(rows < limit, matrix, 0.0)


def prep_kernel(links_ref, place_ref, field_ref, lag_ref, mortar_ref, fold_ref, group_ref, out_ref, flat, line):
    slots = lag_ref.shape[0]
    out_ref[...] = jnp.zeros(out_ref.shape, f32)
    load_flat(flat, field_ref[0, 0, 0])
    line[...] = jnp.zeros(line.shape, f32)
    for s in range(slots):
        line[s : s + 1, : BASIS * BASIS] = lag_ref[s, 0]
    lanes = jnp.broadcast_to(group_ref[0:1, :], (PAD, FLAT))
    rows = lax.broadcasted_iota(jnp.int32, (PAD, FLAT), 0)
    same = rows == lanes
    spreads = [
        jnp.where(same, flat[0:1, :], 0.0),
        jnp.where(same, flat[BASIS - 1 : BASIS, :], 0.0),
        jnp.where(lanes == 0, flat[...], 0.0),
        jnp.where(lanes == BASIS - 1, flat[...], 0.0),
    ]
    for s in range(slots):
        spreads.append(jnp.where(same, line[s : s + 1, :], 0.0))
    parts = []
    for x in spreads:
        parts.extend(split(x))
    out = dot(jnp.concatenate(parts, axis=0), fold_ref[...])
    squares = [out[2 * n * PAD : (2 * n + 1) * PAD] + out[(2 * n + 1) * PAD : (2 * n + 2) * PAD] for n in range(4 + slots)]
    for f in range(4):
        out_ref[0, :, f * PAD : (f + 1) * PAD] = squares[f]
    base = place_ref[0] * slots
    for s in range(slots):
        limits = (links_ref[base + s, 4], links_ref[base + s, 5])
        multiplier = squares[4 + s][:BASIS, :BASIS]
        for side in range(2):
            left = masked(mortar_ref[s, side, 0], limits[0])
            right = masked(mortar_ref[s, side, 1], limits[1])
            half = lax.dot_general(
                left, multiplier, (((0,), (0,)), ((), ())), precision=highest, preferred_element_type=f32
            )
            both = jnp.dot(half, right, precision=highest, preferred_element_type=f32)
            item = 2 * s + side
            at = (item % 4) * PAD
            out_ref[1 + item // 4, :BASIS, at : at + BASIS] = both if side == 0 else -both


def position(mine, other, masks):
    differ = jnp.bitwise_xor(mine, other)
    total = jnp.int32(0)
    for n, mask in enumerate(masks):
        total = total + jnp.where(jnp.bitwise_and(differ, mask) != 0, jnp.int32(1 << n), jnp.int32(0))
    return total


def final_kernel(masks, links_ref, place_ref, *refs):
    rounds = len(masks)
    part_refs = refs[: rounds + 1]
    stiff_a, stiff_b, volume_ref, spread_ref, fold_ref, group_ref, mortar_ref, out_ref, jump_ref, buf, found = refs[rounds + 1 :]
    slots = mortar_ref.shape[0]
    mine = place_ref[0]
    table = links_ref.shape[0]
    buf[0] = part_refs[0][...]
    for n in range(rounds):
        buf[(1 << n) : (2 << n)] = part_refs[n + 1][...].reshape((1 << n,) + buf.shape[1:])
    for f in range(8):
        found[f] = 0

    def look(t, carry):
        for side in range(2):
            hit = jnp.logical_and(links_ref[t, side] == mine, links_ref[t, 4] > 0)
            where = jnp.where(hit, links_ref[t, 2 + side], 4)
            found[where] = 2 * t + side
        return carry

    lax.fori_loop(0, table, look, 0, unroll=8)

    def pick(owner, plane, lane):
        block = buf[position(mine, owner, masks), plane]
        return pltpu.roll(block, lax.rem(WIN - lane * PAD, WIN), axis=1)[:, :PAD]

    squares = []
    for f in range(4):
        item = found[f]
        owner = lax.div(item, 2 * slots)
        item = lax.rem(item, 2 * slots)
        squares.append(pick(owner, 1 + lax.div(item, 4), lax.rem(item, 4)))
    base = mine * slots
    for s in range(slots):
        limits = (links_ref[base + s, 4], links_ref[base + s, 5])
        total = None
        for side in range(2):
            trace = pick(links_ref[base + s, side], 0, links_ref[base + s, 2 + side])
            trace = trace[:BASIS, :BASIS]
            left = masked(mortar_ref[s, side, 0], limits[0])
            right = masked(mortar_ref[s, side, 1], limits[1])
            half = jnp.dot(left, trace, precision=highest, preferred_element_type=f32)
            both = lax.dot_general(
                half, right, (((1,), (1,)), ((), ())), precision=highest, preferred_element_type=f32
            )
            total = both if total is None else total - both
        squares.append(jnp.pad(total, ((0, PAD - BASIS), (0, PAD - BASIS))))
    parts = []
    for x in squares:
        parts.extend(split(x))
    flat = dot_nt(jnp.concatenate(parts, axis=0), fold_ref[...])
    lines = [flat[2 * n * PAD : (2 * n + 1) * PAD] + flat[(2 * n + 1) * PAD : (2 * n + 2) * PAD] for n in range(4 + slots)]
    lanes = jnp.broadcast_to(group_ref[0:1, :], (PAD, FLAT))
    rows = lax.broadcasted_iota(jnp.int32, (PAD, FLAT), 0)
    same = rows == lanes
    for s in range(slots):
        row = jnp.sum(jnp.where(same, lines[4 + s], 0.0), axis=0, keepdims=True)
        jump_ref[s, 0] = row[:, : BASIS * BASIS]
    is_pressure = place_ref[1] == FIELDS - 1
    factor = jnp.where(is_pressure, -stabilize, 1.0).astype(f32)
    total = factor * (stiff_a[...] + stiff_b[...]) - volume_ref[...]
    out = dot_nt(jnp.concatenate(split(total), axis=0), spread_ref[...])
    out = out[:PAD] + out[PAD:]
    low_row = jnp.sum(jnp.where(same, lines[0], 0.0), axis=0, keepdims=True)
    high_row = jnp.sum(jnp.where(same, lines[1], 0.0), axis=0, keepdims=True)
    out = out + jnp.where(rows == 0, low_row, 0.0) + jnp.where(rows == BASIS - 1, high_row, 0.0)
    out = out + jnp.where(lanes == 0, lines[2], 0.0) + jnp.where(lanes == BASIS - 1, lines[3], 0.0)
    out_ref[0, 0, 0] = out[:BASIS, : BASIS * BASIS]


def vmem():
    return pl.BlockSpec(memory_space=pltpu.VMEM)


def smem():
    return pl.BlockSpec(memory_space=pltpu.SMEM)


def anywhere():
    return pl.BlockSpec(memory_space=pl.ANY)


params = pltpu.CompilerParams(vmem_limit_bytes=48 << 20)


def stiff_call(groups, expand_here, field, tables, weight):
    count = 4 * len(groups)
    scratch = [
        pltpu.VMEM((QUAD, count * SPAN), f32),
        pltpu.VMEM((count * PAD, 3 * SPAN), bf16),
        pltpu.VMEM((count * PAD, 3 * SPAN), bf16),
        pltpu.VMEM((2 * count * PAD, 3 * SPAN), bf16),
        pltpu.SemaphoreType.DMA((len(groups),)),
    ]
    wide = jax.ShapeDtypeStruct((PAD, WIDE), f32)
    if expand_here:
        scratch = [pltpu.VMEM((PAD, FLAT), f32)] + scratch
    return pl.pallas_call(
        functools.partial(stiff_kernel, groups, expand_here),
        out_shape=(wide, wide) if expand_here else wide,
        in_specs=[vmem()] * 6 + [anywhere()],
        out_specs=(vmem(), vmem()) if expand_here else vmem(),
        scratch_shapes=scratch,
        compiler_params=params,
    )(field, tables["spread"], tables["ahead"], tables["outer"], tables["inner"], tables["back"], weight)


def volume_call(place, near, far, tables, weight):
    return pl.pallas_call(
        volume_kernel,
        out_shape=jax.ShapeDtypeStruct((PAD, WIDE), f32),
        in_specs=[smem()] + [vmem()] * 7 + [anywhere()],
        out_specs=vmem(),
        scratch_shapes=[
            pltpu.VMEM((3, PAD, FLAT), f32),
            pltpu.VMEM((QUAD, ELEMS * SPAN), f32),
            pltpu.VMEM((ELEMS * PAD, 2 * SPAN), bf16),
            pltpu.VMEM((ELEMS * PAD, 2 * SPAN), bf16),
            pltpu.VMEM((2 * ELEMS * PAD, SPAN), bf16),
            pltpu.SemaphoreType.DMA((GROUPS,)),
        ],
        compiler_params=params,
    )(place, near, far, tables["spread"], tables["ahead"], tables["outer"], tables["inner"], tables["back"], weight)


def swap(array, axis, mask):
    size = lax.axis_size(axis)
    return lax.ppermute(array, axis, [(n, n ^ mask) for n in range(size)])


def per_device(state, stiff_weight, volume_weight, lagrange, mortar, links):
    tables = {name: jnp.asarray(value) for name, value in constants().items()}
    patches = lax.axis_size("patch")
    place = jnp.stack([lax.axis_index("patch"), lax.axis_index("sub")]).astype(jnp.int32)
    slots = mortar.shape[0]
    planes = 1 + (2 * slots + 3) // 4
    masks = [1 << n for n in reversed(range(patches.bit_length() - 1))]

    near = swap(state, "sub", 1)
    far = swap(jnp.concatenate([state[0, 0], near[0, 0]], axis=0), "sub", 2)
    own = pl.pallas_call(
        prep_kernel,
        out_shape=jax.ShapeDtypeStruct((planes, PAD, WIN), f32),
        in_specs=[smem(), smem()] + [vmem()] * 5,
        out_specs=vmem(),
        scratch_shapes=[pltpu.VMEM((PAD, FLAT), f32), pltpu.VMEM((8, FLAT), f32)],
        compiler_params=params,
    )(links, place, state, lagrange, mortar, tables["fold"], tables["group"])
    parts = [own]
    held = own
    for mask in masks:
        other = swap(held, "patch", mask)
        parts.append(other)
        held = jnp.concatenate([held, other], axis=0)

    half = GROUPS // 2
    stiff_a, wide = stiff_call(list(range(half)), True, state, tables, stiff_weight)
    stiff_b = stiff_call(list(range(half, GROUPS)), False, wide, tables, stiff_weight)
    volume = volume_call(place, near, far, tables, volume_weight)
    return pl.pallas_call(
        functools.partial(final_kernel, masks),
        out_shape=(
            jax.ShapeDtypeStruct(state.shape, f32),
            jax.ShapeDtypeStruct((slots, 1, 1, BASIS * BASIS), f32),
        ),
        in_specs=[smem(), smem()] + [vmem()] * (len(parts) + 7),
        out_specs=(vmem(), vmem()),
        scratch_shapes=[pltpu.VMEM((patches, planes, PAD, WIN), f32), pltpu.SMEM((8,), jnp.int32)],
        compiler_params=params,
    )(links, place, *parts, stiff_a, stiff_b, volume, tables["spread"], tables["fold"], tables["group"], mortar)


def solution(mesh):
    return jax.shard_map(
        per_device,
        mesh=mesh,
        in_specs=(
            P("patch", "sub", None, None, None),
            P("patch", None, None),
            P("patch", None, None),
            P("patch", "sub", None, None),
            P("patch", None, None, None, None),
            P(),
        ),
        out_specs=(P("patch", "sub", None, None, None), P("patch", "sub", None, None)),
        check_vma=False,
    )
```

```python
import functools

import jax
import jax.numpy as jnp
import numpy as np
from jax import lax
from jax.experimental import pallas as pl
from jax.experimental.pallas import tpu as pltpu
from jax.sharding import PartitionSpec as P


ELEMS = 24
DEGREE = 3
FIELDS = 4
LOCAL = DEGREE + 1
NODES = 4
BASIS = ELEMS + DEGREE
QUAD = ELEMS * NODES
PAD = 32
WIN = LOCAL * PAD
SPAN = NODES * QUAD
GROUPS = ELEMS // 4
WIDE = (GROUPS + 1) * WIN
FLAT = 768
GROUP_ROWS = 4 * PAD

stabilize = 0.25
f32 = jnp.float32
bf16 = jnp.bfloat16
gauss_points_four = [
    -0.8611363115940526,
    -0.3399810435848563,
    0.3399810435848563,
    0.8611363115940526,
]
gauss_weights_four = [
    0.3478548451374538,
    0.6521451548625461,
    0.6521451548625461,
    0.3478548451374538,
]


def spline_tables(knot_list, points, degree):
    current = np.where(
        (knot_list[None, :-1] <= points[:, None]) & (points[:, None] < knot_list[None, 1:]),
        1.0,
        0.0,
    )
    previous = current
    for order_k in range(1, degree + 1):
        previous = current
        amount = len(knot_list) - 1 - order_k
        current = np.zeros((points.shape[0], amount))
        for column in range(amount):
            left_span = knot_list[column + order_k] - knot_list[column]
            right_span = knot_list[column + order_k + 1] - knot_list[column + 1]
            if left_span > 0:
                current[:, column] += (points - knot_list[column]) / left_span * previous[:, column]
            if right_span > 0:
                current[:, column] += (
                    (knot_list[column + order_k + 1] - points)
                    / right_span
                    * previous[:, column + 1]
                )
    slope_part = np.zeros(current.shape)
    for column in range(current.shape[1]):
        left_span = knot_list[column + degree] - knot_list[column]
        right_span = knot_list[column + degree + 1] - knot_list[column + 1]
        if left_span > 0:
            slope_part[:, column] += degree / left_span * previous[:, column]
        if right_span > 0:
            slope_part[:, column] -= degree / right_span * previous[:, column + 1]
    return current, slope_part


def halves(table):
    high = table.astype(np.dtype(bf16)).astype(np.float64)
    return high, table - high


def padded(table, rows, cols):
    out = np.zeros((rows, cols))
    out[: table.shape[0], : table.shape[1]] = table
    return out


@functools.cache
def constants():
    nodes = np.array(gauss_points_four)
    points = (np.arange(ELEMS)[:, None] + (nodes[None, :] + 1.0) / 2.0).reshape(-1)
    weights = np.tile(np.array(gauss_weights_four) / 2.0, ELEMS)
    open_knots = np.concatenate(
        [np.zeros(DEGREE), np.arange(ELEMS + 1.0), np.full(DEGREE, float(ELEMS))]
    )
    even_knots = np.arange(-DEGREE, ELEMS + DEGREE + 1.0)
    value, slope = spline_tables(open_knots, points, DEGREE)
    even_value, even_slope = spline_tables(even_knots, points, DEGREE)
    change = np.round(np.linalg.lstsq(even_value, value, rcond=None)[0] * 4.0) / 4.0
    local_value = even_value[4 * NODES : 5 * NODES, 4 : 4 + LOCAL]
    local_slope = even_slope[4 * NODES : 5 * NODES, 4 : 4 + LOCAL]
    local_w = weights[:NODES, None]

    def kron(local, table):
        wide = padded(table, QUAD, PAD)
        return np.einsum("bj,ck->jkbc", local, wide).reshape(WIN, SPAN)

    ahead = np.concatenate(
        [kron(local_value, value), kron(local_slope, value), kron(local_value, slope)], axis=1
    )
    value_w, slope_w = value * weights[:, None], slope * weights[:, None]
    back = np.concatenate(
        [
            kron(local_value * local_w, value_w).T,
            kron(local_slope * local_w, value_w).T,
            kron(local_value * local_w, slope_w).T,
        ],
        axis=0,
    )
    ahead_high, ahead_low = halves(ahead)
    ahead3 = np.concatenate([ahead_high, ahead_high, ahead_low], axis=0)
    back_high, back_low = halves(back)
    back2 = np.concatenate([back_high, back_low], axis=1)

    def left3(table):
        high, low = halves(padded(table, QUAD, PAD))
        return np.concatenate([high, high, low], axis=1)

    def left4(table):
        high, low = halves(padded(table, QUAD, PAD).T)
        return np.concatenate(
            [np.concatenate([high, high], axis=1), np.concatenate([low, low], axis=1)], axis=0
        )

    spread = np.zeros((BASIS, BASIS, WIDE // PAD, PAD))
    for k in range(BASIS):
        spread[:, k, :BASIS, k] = change.T
    spread = padded(spread.reshape(BASIS * BASIS, WIDE), FLAT, WIDE)
    as16 = lambda a: a.astype(np.dtype(bf16))
    return dict(
        ahead=as16(ahead3),
        back=as16(back2),
        outer=as16(np.stack([left3(slope), left3(value)])),
        inner=as16(np.stack([left4(slope_w), left4(value_w)])),
        spread=as16(spread),
    )


def split(x):
    high = x.astype(bf16)
    return high, (x - high.astype(f32)).astype(bf16)


def dot(a, b):
    return jnp.dot(a, b, preferred_element_type=f32)


def dot_nt(a, b):
    return lax.dot_general(a, b, (((1,), (1,)), ((), ())), preferred_element_type=f32)


def expand(fields, spread):
    parts = []
    for field in fields:
        parts.extend(split(field))
    out = dot(jnp.concatenate(parts, axis=0), spread)
    return halves_sum(out, len(fields))


def halves_sum(out, count):
    return [
        out[2 * n * PAD : (2 * n + 1) * PAD] + out[(2 * n + 1) * PAD : (2 * n + 2) * PAD]
        for n in range(count)
    ]


def shifts(wide):
    rolled = [wide] + [pltpu.roll(wide, WIDE - PAD * r, axis=1) for r in range(1, 4)]
    return [split(x) for x in rolled]


def windows(shifted, m):
    rows = []
    for r in range(4):
        high = shifted[r][0][:, m * WIN : (m + 1) * WIN]
        low = shifted[r][1][:, m * WIN : (m + 1) * WIN]
        rows.append(jnp.concatenate([high, low, high], axis=1))
    return jnp.concatenate(rows, axis=0)


def overlap(rows, groups):
    first, count = groups[0], len(groups)
    total = None
    for r in range(4):
        pieces = []
        if first > 0:
            pieces.append(jnp.zeros((PAD, first * WIN), f32))
        pieces.extend(rows[n][r * PAD : (r + 1) * PAD] for n in range(count))
        rest = WIDE // WIN - first - count
        pieces.append(jnp.zeros((PAD, rest * WIN), f32))
        line = jnp.concatenate(pieces, axis=1)
        if r > 0:
            line = pltpu.roll(line, PAD * r, axis=1)
        total = line if total is None else total + line
    return total


def gather_back(heads_ref, n, back):
    high = heads_ref[n * GROUP_ROWS : (n + 1) * GROUP_ROWS, :]
    low = heads_ref[heads_ref.shape[0] // 2 + n * GROUP_ROWS : heads_ref.shape[0] // 2 + (n + 1) * GROUP_ROWS, :]
    out = dot(jnp.concatenate([high, low], axis=0), back)
    out = out[:GROUP_ROWS] + out[GROUP_ROWS:]
    return out[:, :WIN] + out[:, WIN:]


def load_flat(dst, src):
    dst[...] = jnp.zeros(dst.shape, f32)
    for i in range(BASIS):
        dst[i : i + 1, : BASIS * BASIS] = src[i]


def element_pairs(groups, ahead, outers, inners, planes, back, weight_ref, base, mid_h, mid_l, prod, heads):
    count = len(groups)
    pairs = 2 * count
    half = heads.shape[0] // 2
    done = []

    def forward(p):
        scale = [weight_ref[:, base + (2 * p + q) * SPAN : base + (2 * p + q + 1) * SPAN] for q in range(2)]
        column = 0
        for outer, sources in zip(outers, planes):
            pieces = []
            for q in range(2):
                row = (2 * p + q) * PAD
                for source in sources:
                    stack = []
                    for block in source:
                        cols = slice(block * SPAN, (block + 1) * SPAN)
                        stack += [mid_h[row : row + PAD, cols], mid_l[row : row + PAD, cols], mid_h[row : row + PAD, cols]]
                    pieces.append(jnp.concatenate(stack, axis=0))
            out = dot(outer, jnp.concatenate(pieces, axis=1))
            wide = jnp.concatenate([scale[q] for q in range(2) for _ in sources], axis=1)
            high, low = split(out * wide)
            width = 2 * len(sources) * SPAN
            prod[p % 2, :QUAD, column : column + width] = high
            prod[p % 2, QUAD:, column : column + width] = low
            column += width

    def backward(p):
        column = 0
        place = 0
        for inner, sources in zip(inners, planes):
            width = 2 * len(sources) * SPAN
            out = dot(inner, prod[p % 2, :, column : column + width])
            high, low = split(out[:PAD] + out[PAD:])
            for q in range(2):
                row = (2 * p + q) * PAD
                take = slice(q * len(sources) * SPAN, (q + 1) * len(sources) * SPAN)
                put = slice(place, place + len(sources) * SPAN)
                heads[row : row + PAD, put] = high[:, take]
                heads[half + row : half + row + PAD, put] = low[:, take]
            column += width
            place += len(sources) * SPAN

    ahead(0)
    for p in range(pairs + 1):
        if p < pairs:
            forward(p)
            if p % 2 == 0 and p // 2 + 1 < count:
                ahead(p // 2 + 1)
        if p > 0:
            backward(p - 1)
        if p >= 3 and p % 2 == 1:
            done.append(gather_back(heads, len(done), back))
    while len(done) < count:
        done.append(gather_back(heads, len(done), back))
    return overlap(done, groups)


def start_all(pairs, sems):
    copies = [pltpu.make_async_copy(src, dst, sems.at[n]) for n, (src, dst) in enumerate(pairs)]
    for copy in copies:
        copy.start()
    return copies


def stiff_kernel(groups, fetch_lanes, wide_ref, ahead_ref, outer_ref, inner_ref, back_ref, weight_ref, next_hbm, out_ref, next_ref, mid_h, mid_l, prod, heads, sems):
    copies = start_all([(next_hbm.at[0, :, fetch_lanes], next_ref)], sems)
    shifted = shifts(wide_ref[...])

    def ahead(n):
        high, low = split(dot(windows(shifted, groups[n]), ahead_ref[...]))
        mid_h[n * GROUP_ROWS : (n + 1) * GROUP_ROWS, :] = high
        mid_l[n * GROUP_ROWS : (n + 1) * GROUP_ROWS, :] = low

    out_ref[...] = element_pairs(
        groups,
        ahead,
        (outer_ref[0], outer_ref[1]),
        (inner_ref[0], inner_ref[1]),
        (((0,),), ((1,), (2,))),
        back_ref[...],
        weight_ref,
        0,
        mid_h,
        mid_l,
        prod,
        heads,
    )
    for copy in copies:
        copy.wait()


def volume_kernel(near_ref, far_ref, spread_ref, ahead_ref, outer_ref, inner_ref, back_ref, weight_ref, stiff_a, stiff_b, out_ref, flat, mid_h, mid_l, prod, heads):
    groups = list(range(GROUPS))
    sub = lax.axis_index("sub")
    is_pressure = sub == FIELDS - 1
    load_flat(flat.at[0], near_ref)
    load_flat(flat.at[1], far_ref.at[0])
    load_flat(flat.at[2], far_ref.at[1])
    chosen = jnp.where(is_pressure, 2, 2 - sub)
    zero = jnp.zeros((PAD, FLAT), f32)
    fields = [
        flat[chosen],
        jnp.where(is_pressure, flat[1], zero),
        jnp.where(is_pressure, flat[0], zero),
    ]
    shifted = [shifts(wide) for wide in expand(fields, spread_ref[...])]

    def ahead(n):
        at = slice(n * GROUP_ROWS, (n + 1) * GROUP_ROWS)
        mid = dot(windows(shifted[0], groups[n]), ahead_ref[:, :SPAN])
        high, low = split(mid)
        mid_h[at, :SPAN] = high
        mid_l[at, :SPAN] = low
        mid = dot(windows(shifted[1], groups[n]), ahead_ref[:, SPAN : 2 * SPAN]) + dot(
            windows(shifted[2], groups[n]), ahead_ref[:, 2 * SPAN :]
        )
        high, low = split(mid)
        mid_h[at, SPAN:] = high
        mid_l[at, SPAN:] = low

    along = jnp.where(is_pressure, 0, 1)
    outer = jnp.concatenate([outer_ref[along], outer_ref[1]], axis=1)
    inner = inner_ref[jnp.where(sub == 0, 0, 1)]
    kind = jnp.where(is_pressure, 0, sub)
    back = back_ref[pl.ds(pl.multiple_of(kind * SPAN, SPAN), SPAN), :]
    volume = element_pairs(
        groups, ahead, (outer,), (inner,), (((0, 1),),), back, weight_ref, 0, mid_h, mid_l, prod, heads
    )
    factor = jnp.where(is_pressure, -stabilize, 1.0).astype(f32)
    total = factor * (stiff_a[...] + stiff_b[...]) - volume
    out = dot_nt(jnp.concatenate(split(total), axis=0), spread_ref[...])
    out_ref[...] = out[:PAD] + out[PAD:]


def masked(matrix, limit):
    rows = lax.broadcasted_iota(jnp.int32, matrix.shape, 0)
    return jnp.where(rows < limit, matrix, 0.0)


def layers():
    lanes = lax.broadcasted_iota(jnp.int32, (PAD, FLAT), 1)
    group = jnp.floor((lanes.astype(f32) + 0.5) * (1.0 / BASIS)).astype(jnp.int32)
    rows = lax.broadcasted_iota(jnp.int32, (PAD, FLAT), 0)
    inside = lanes - BASIS * group == rows
    return group, rows, jnp.where(inside, 1.0, 0.0).astype(bf16)


def dot_split(a, b, dims):
    a_high, a_low = split(a)
    b_high, b_low = split(b)
    dims = (dims, ((), ()))
    general = functools.partial(lax.dot_general, dimension_numbers=dims, preferred_element_type=f32)
    return general(a_high, b_high) + (general(a_high, b_low) + general(a_low, b_high))


def prep_kernel(links_hbm, field_hbm, lag_hbm, mortar_hbm, spread_hbm, ahead_hbm, outer_hbm, inner_hbm, back_hbm, weight_hbm, own_ref, wide_ref, spread_ref, ahead_ref, outer_ref, inner_ref, back_ref, weight_ref, links, field, lag, mortar, flat, line, sems):
    copies = start_all(
        [
            (field_hbm, field),
            (lag_hbm, lag),
            (links_hbm, links),
            (mortar_hbm, mortar),
            (spread_hbm, spread_ref),
            (ahead_hbm, ahead_ref),
            (outer_hbm, outer_ref),
            (inner_hbm, inner_ref),
            (back_hbm, back_ref),
            (weight_hbm.at[0, :, pl.ds(0, weight_ref.shape[1])], weight_ref),
        ],
        sems,
    )
    slots = lag.shape[0]
    own_ref[...] = jnp.zeros(own_ref.shape, f32)
    line[...] = jnp.zeros(line.shape, f32)
    group, rows, fold = layers()
    same = rows == group
    for copy in copies[:4]:
        copy.wait()
    load_flat(flat, field)
    for s in range(slots):
        line[s : s + 1, : BASIS * BASIS] = lag[s, 0]
    spreads = [jnp.where(same, line[s : s + 1, :], 0.0) for s in range(slots)]
    spreads += [
        jnp.where(same, flat[0:1, :], 0.0),
        jnp.where(same, flat[BASIS - 1 : BASIS, :], 0.0),
        jnp.where(group == 0, flat[...], 0.0),
        jnp.where(group == BASIS - 1, flat[...], 0.0),
    ]
    parts = []
    for x in spreads:
        parts.extend(split(x))
    squares = halves_sum(dot_nt(jnp.concatenate(parts, axis=0), fold), 4 + slots)
    base = lax.axis_index("patch") * slots
    halfway = []
    for s in range(slots):
        for side in range(2):
            left = masked(mortar[s, side, :, 0, :], links[4, base + s])
            halfway.append(dot_split(left, squares[s][:BASIS, :BASIS], ((0,), (0,))))
    for s in range(slots):
        for side in range(2):
            right = masked(mortar[s, side, :, 1, :], links[5, base + s])
            both = dot_split(halfway[2 * s + side], right, ((1,), (0,)))
            item = 2 * s + side
            at = (item % 4) * PAD
            own_ref[1 + item // 4, :BASIS, at : at + BASIS] = both if side == 0 else -both
    for f in range(4):
        own_ref[0, :, f * PAD : (f + 1) * PAD] = squares[slots + f]
    copies[4].wait()
    (wide,) = expand([flat[...]], spread_ref[...])
    wide_ref[...] = wide
    for copy in copies[5:]:
        copy.wait()


def position(mine, other, masks):
    differ = jnp.bitwise_xor(mine, other)
    total = jnp.int32(0)
    for n, mask in enumerate(masks):
        total = total + jnp.where(jnp.bitwise_and(differ, mask) != 0, jnp.int32(1 << n), jnp.int32(0))
    return total


def final_kernel(masks, links_hbm, mortar_hbm, *refs):
    rounds = len(masks)
    part_refs = refs[: rounds + 1]
    inner_ref, out_ref, jump_ref, buf, links, mortar, found, sems = refs[rounds + 1 :]
    copies = start_all([(links_hbm, links), (mortar_hbm, mortar)], sems)
    slots = mortar.shape[0]
    mine = lax.axis_index("patch")
    table = links.shape[1]
    buf[0] = part_refs[0][...]
    for n in range(rounds):
        buf[(1 << n) : (2 << n)] = part_refs[n + 1][...].reshape((1 << n,) + buf.shape[1:])
    group, rows, fold = layers()
    same = rows == group
    for f in range(5):
        found[f] = 0
    for copy in copies:
        copy.wait()

    def look(t, carry):
        for side in range(2):
            hit = jnp.logical_and(links[side, t] == mine, links[4, t] > 0)
            found[jnp.where(hit, links[2 + side, t], 4)] = 2 * t + side
        return carry

    def pick(owner, plane, lane):
        block = buf[position(mine, owner, masks), plane]
        return pltpu.roll(block, lax.rem(WIN - lane * PAD, WIN), axis=1)[:, :PAD]

    base = mine * slots
    halfway = []
    for s in range(slots):
        for side in range(2):
            trace = pick(links[side, base + s], 0, links[2 + side, base + s])
            left = masked(mortar[s, side, :, 0, :], links[4, base + s])
            halfway.append(dot_split(left, trace[:BASIS, :BASIS], ((1,), (0,))))
    jumps = []
    for s in range(slots):
        total = None
        for side in range(2):
            right = masked(mortar[s, side, :, 1, :], links[5, base + s])
            both = dot_split(halfway[2 * s + side], right, ((1,), (1,)))
            total = both if total is None else total - both
        jumps.append(jnp.pad(total, ((0, PAD - BASIS), (0, PAD - BASIS))))
    if table <= 64:
        for t in range(table):
            look(t, 0)
    else:
        lax.fori_loop(0, table, look, 0, unroll=8)
    squares = []
    for f in range(4):
        item = found[f]
        owner = lax.div(item, 2 * slots)
        item = lax.rem(item, 2 * slots)
        squares.append(pick(owner, 1 + lax.div(item, 4), lax.rem(item, 4)))
    parts = []
    for x in squares + jumps:
        parts.extend(split(x))
    lines = halves_sum(dot(jnp.concatenate(parts, axis=0), fold), 4 + slots)
    out = inner_ref[...]
    low_row = jnp.sum(jnp.where(same, lines[0], 0.0), axis=0, keepdims=True)
    high_row = jnp.sum(jnp.where(same, lines[1], 0.0), axis=0, keepdims=True)
    out = out + jnp.where(rows == 0, low_row, 0.0) + jnp.where(rows == BASIS - 1, high_row, 0.0)
    out = out + jnp.where(group == 0, lines[2], 0.0) + jnp.where(group == BASIS - 1, lines[3], 0.0)
    for i in range(BASIS):
        out_ref[i] = out[i : i + 1, : BASIS * BASIS]
    for s in range(slots):
        row = jnp.sum(jnp.where(same, lines[4 + s], 0.0), axis=0, keepdims=True)
        jump_ref[s, 0] = row[:, : BASIS * BASIS]


def vmem():
    return pl.BlockSpec(memory_space=pltpu.VMEM)


def anywhere():
    return pl.BlockSpec(memory_space=pltpu.HBM)


def in_hbm(*arrays):
    return [pltpu.with_memory_space_constraint(x, pltpu.HBM) for x in arrays]


params = pltpu.CompilerParams(vmem_limit_bytes=24 << 20)
halfspan = (GROUPS // 2) * 4 * SPAN


def stiff_call(groups, fetch, wide, tables, weight, following):
    count = 4 * len(groups)
    lanes = pl.ds(fetch[0], fetch[1])
    return pl.pallas_call(
        functools.partial(stiff_kernel, groups, lanes),
        out_shape=(
            jax.ShapeDtypeStruct((PAD, WIDE), f32),
            jax.ShapeDtypeStruct((QUAD, fetch[1]), f32),
        ),
        in_specs=[vmem()] * 6 + [anywhere()],
        out_specs=(vmem(), vmem()),
        scratch_shapes=[
            pltpu.VMEM((count * PAD, 3 * SPAN), bf16),
            pltpu.VMEM((count * PAD, 3 * SPAN), bf16),
            pltpu.VMEM((2, 2 * QUAD, 6 * SPAN), bf16),
            pltpu.VMEM((2 * count * PAD, 3 * SPAN), bf16),
            pltpu.SemaphoreType.DMA((1,)),
        ],
        compiler_params=params,
    )(wide, *tables[1:], weight, *in_hbm(following))


def volume_call(near, far, tables, weight, stiff_a, stiff_b):
    return pl.pallas_call(
        volume_kernel,
        out_shape=jax.ShapeDtypeStruct((PAD, FLAT), f32),
        in_specs=[vmem()] * 10,
        out_specs=vmem(),
        scratch_shapes=[
            pltpu.VMEM((3, PAD, FLAT), f32),
            pltpu.VMEM((ELEMS * PAD, 2 * SPAN), bf16),
            pltpu.VMEM((ELEMS * PAD, 2 * SPAN), bf16),
            pltpu.VMEM((2, 2 * QUAD, 2 * SPAN), bf16),
            pltpu.VMEM((2 * ELEMS * PAD, SPAN), bf16),
        ],
        compiler_params=params,
    )(near, far, *tables, weight, stiff_a, stiff_b)


def prep_call(links, field, lagrange, mortar, tables, stiff_weight, planes):
    return pl.pallas_call(
        prep_kernel,
        out_shape=(
            jax.ShapeDtypeStruct((planes, PAD, WIN), f32),
            jax.ShapeDtypeStruct((PAD, WIDE), f32),
            *(jax.ShapeDtypeStruct(t.shape, bf16) for t in tables),
            jax.ShapeDtypeStruct((QUAD, halfspan), f32),
        ),
        in_specs=[anywhere()] * 10,
        out_specs=(vmem(),) * 8,
        scratch_shapes=[
            pltpu.SMEM(links.shape, jnp.int32),
            pltpu.VMEM(field.shape, f32),
            pltpu.VMEM(lagrange.shape, f32),
            pltpu.VMEM(mortar.shape, f32),
            pltpu.VMEM((PAD, FLAT), f32),
            pltpu.VMEM((8, FLAT), f32),
            pltpu.SemaphoreType.DMA((10,)),
        ],
        compiler_params=params,
    )(*in_hbm(links, field, lagrange, mortar, *tables, stiff_weight))


def swap(array, axis, mask):
    size = lax.axis_size(axis)
    return lax.ppermute(array, axis, [(n, n ^ mask) for n in range(size)])


def after(array, *others):
    return lax.optimization_barrier((array,) + others)[0]


def per_device(state, stiff_weight, volume_weight, lagrange, mortar, links):
    tables = [jnp.asarray(constants()[name]) for name in ("spread", "ahead", "outer", "inner", "back")]
    patches = lax.axis_size("patch")
    slots = mortar.shape[0]
    planes = 1 + (2 * slots + 3) // 4
    masks = [1 << n for n in reversed(range(patches.bit_length() - 1))]
    field = jnp.transpose(state, (0, 1, 3, 2, 4))[0, 0]
    mortar = jnp.transpose(mortar, (0, 1, 3, 2, 4))
    links = links.T

    near = swap(field, "sub", 1)
    own, wide, *tables, weight_a = prep_call(links, field, lagrange, mortar, tables, stiff_weight, planes)
    far = swap(jnp.stack([field, near]), "sub", 2)
    first = GROUPS // 2
    stiff_a, weight_b = stiff_call(
        list(range(first)), (halfspan, ELEMS * SPAN - halfspan), wide, tables, weight_a, stiff_weight
    )
    stiff_b, weight_c = stiff_call(
        list(range(first, GROUPS)), (0, ELEMS * SPAN), wide, tables, weight_b, volume_weight
    )
    inner = volume_call(near, far, tables, weight_c, stiff_a, stiff_b)
    gates = [None, stiff_a, stiff_b]
    parts = [own]
    held = own
    for n, mask in enumerate(masks):
        late = len(masks) - n
        gate = gates[max(0, 3 - late)] if n > 0 else None
        other = swap(held if gate is None else after(held, gate), "patch", mask)
        parts.append(other)
        held = jnp.concatenate([held, other], axis=0)
    residual, constraint = pl.pallas_call(
        functools.partial(final_kernel, masks),
        out_shape=(
            jax.ShapeDtypeStruct(field.shape, f32),
            jax.ShapeDtypeStruct((slots, 1, 1, BASIS * BASIS), f32),
        ),
        in_specs=[anywhere(), anywhere()] + [vmem()] * (len(parts) + 1),
        out_specs=(vmem(), vmem()),
        scratch_shapes=[
            pltpu.VMEM((patches, planes, PAD, WIN), f32),
            pltpu.SMEM(links.shape, jnp.int32),
            pltpu.VMEM(mortar.shape, f32),
            pltpu.SMEM((8,), jnp.int32),
            pltpu.SemaphoreType.DMA((2,)),
        ],
        compiler_params=params,
    )(*in_hbm(links, mortar), *parts, inner)
    return jnp.transpose(residual[None, None], (0, 1, 3, 2, 4)), constraint


def solution(mesh):
    return jax.shard_map(
        per_device,
        mesh=mesh,
        in_specs=(
            P("patch", "sub", None, None, None),
            P("patch", None, None),
            P("patch", None, None),
            P("patch", "sub", None, None),
            P("patch", None, None, None, None),
            P(),
        ),
        out_specs=(P("patch", "sub", None, None, None), P("patch", "sub", None, None)),
        check_vma=False,
    )
```

```python
import functools

import jax
import jax.numpy as jnp
import numpy as np
from jax import lax
from jax.experimental import pallas as pl
from jax.experimental.pallas import tpu as pltpu
from jax.sharding import PartitionSpec as P


ELEMS = 24
DEGREE = 3
FIELDS = 4
LOCAL = DEGREE + 1
NODES = 4
BASIS = ELEMS + DEGREE
QUAD = ELEMS * NODES
PAD = 32
WIN = LOCAL * PAD
SPAN = NODES * QUAD
GROUPS = ELEMS // 4
EARLY = GROUPS - 2
WIDE = (GROUPS + 1) * WIN
FLAT = 768
GROUP_ROWS = 4 * PAD

stabilize = 0.25
f32 = jnp.float32
bf16 = jnp.bfloat16
gauss_points_four = [
    -0.8611363115940526,
    -0.3399810435848563,
    0.3399810435848563,
    0.8611363115940526,
]
gauss_weights_four = [
    0.3478548451374538,
    0.6521451548625461,
    0.6521451548625461,
    0.3478548451374538,
]


def spline_tables(knot_list, points, degree):
    current = np.where(
        (knot_list[None, :-1] <= points[:, None]) & (points[:, None] < knot_list[None, 1:]),
        1.0,
        0.0,
    )
    previous = current
    for order_k in range(1, degree + 1):
        previous = current
        amount = len(knot_list) - 1 - order_k
        current = np.zeros((points.shape[0], amount))
        for column in range(amount):
            left_span = knot_list[column + order_k] - knot_list[column]
            right_span = knot_list[column + order_k + 1] - knot_list[column + 1]
            if left_span > 0:
                current[:, column] += (points - knot_list[column]) / left_span * previous[:, column]
            if right_span > 0:
                current[:, column] += (
                    (knot_list[column + order_k + 1] - points)
                    / right_span
                    * previous[:, column + 1]
                )
    slope_part = np.zeros(current.shape)
    for column in range(current.shape[1]):
        left_span = knot_list[column + degree] - knot_list[column]
        right_span = knot_list[column + degree + 1] - knot_list[column + 1]
        if left_span > 0:
            slope_part[:, column] += degree / left_span * previous[:, column]
        if right_span > 0:
            slope_part[:, column] -= degree / right_span * previous[:, column + 1]
    return current, slope_part


def halves(table):
    high = table.astype(np.dtype(bf16)).astype(np.float64)
    return high, table - high


def padded(table, rows, cols):
    out = np.zeros((rows, cols))
    out[: table.shape[0], : table.shape[1]] = table
    return out


@functools.cache
def constants():
    nodes = np.array(gauss_points_four)
    points = (np.arange(ELEMS)[:, None] + (nodes[None, :] + 1.0) / 2.0).reshape(-1)
    weights = np.tile(np.array(gauss_weights_four) / 2.0, ELEMS)
    open_knots = np.concatenate(
        [np.zeros(DEGREE), np.arange(ELEMS + 1.0), np.full(DEGREE, float(ELEMS))]
    )
    even_knots = np.arange(-DEGREE, ELEMS + DEGREE + 1.0)
    value, slope = spline_tables(open_knots, points, DEGREE)
    even_value, even_slope = spline_tables(even_knots, points, DEGREE)
    change = np.round(np.linalg.lstsq(even_value, value, rcond=None)[0] * 4.0) / 4.0
    local_value = even_value[4 * NODES : 5 * NODES, 4 : 4 + LOCAL]
    local_slope = even_slope[4 * NODES : 5 * NODES, 4 : 4 + LOCAL]
    local_w = weights[:NODES, None]

    def kron(local, table):
        wide = padded(table, QUAD, PAD)
        return np.einsum("bj,ck->jkbc", local, wide).reshape(WIN, SPAN)

    ahead = np.concatenate(
        [kron(local_value, value), kron(local_slope, value), kron(local_value, slope)], axis=1
    )
    value_w, slope_w = value * weights[:, None], slope * weights[:, None]
    back = np.concatenate(
        [
            kron(local_value * local_w, value_w).T,
            kron(local_slope * local_w, value_w).T,
            kron(local_value * local_w, slope_w).T,
        ],
        axis=0,
    )
    ahead_high, ahead_low = halves(ahead)
    ahead3 = np.concatenate([ahead_high, ahead_high, ahead_low], axis=0)
    back_high, back_low = halves(back)
    back2 = np.concatenate([back_high, back_low], axis=1)

    def left3(table):
        high, low = halves(padded(table, QUAD, PAD))
        return np.concatenate([high, high, low], axis=1)

    def left4(table):
        high, low = halves(padded(table, QUAD, PAD).T)
        return np.concatenate(
            [np.concatenate([high, high], axis=1), np.concatenate([low, low], axis=1)], axis=0
        )

    spread = np.zeros((BASIS, BASIS, WIDE // PAD, PAD))
    for k in range(BASIS):
        spread[:, k, :BASIS, k] = change.T
    spread = padded(spread.reshape(BASIS * BASIS, WIDE), FLAT, WIDE)
    as16 = lambda a: a.astype(np.dtype(bf16))
    return dict(
        ahead=as16(ahead3),
        back=as16(back2),
        outer=as16(np.stack([left3(slope), left3(value)])),
        inner=as16(np.stack([left4(slope_w), left4(value_w)])),
        spread=as16(spread),
    )


def split(x):
    high = x.astype(bf16)
    return high, (x - high.astype(f32)).astype(bf16)


def dot(a, b):
    return jnp.dot(a, b, preferred_element_type=f32)


def dot_nt(a, b):
    return lax.dot_general(a, b, (((1,), (1,)), ((), ())), preferred_element_type=f32)


def expand(fields, spread):
    parts = []
    for field in fields:
        parts.extend(split(field))
    out = dot(jnp.concatenate(parts, axis=0), spread)
    return halves_sum(out, len(fields))


def halves_sum(out, count):
    return [
        out[2 * n * PAD : (2 * n + 1) * PAD] + out[(2 * n + 1) * PAD : (2 * n + 2) * PAD]
        for n in range(count)
    ]


def shifts(wide):
    rolled = [wide] + [pltpu.roll(wide, WIDE - PAD * r, axis=1) for r in range(1, 4)]
    return [split(x) for x in rolled]


def windows(shifted, m):
    rows = []
    for r in range(4):
        high = shifted[r][0][:, m * WIN : (m + 1) * WIN]
        low = shifted[r][1][:, m * WIN : (m + 1) * WIN]
        rows.append(jnp.concatenate([high, low, high], axis=1))
    return jnp.concatenate(rows, axis=0)


def overlap(rows, groups):
    first, count = groups[0], len(groups)
    total = None
    for r in range(4):
        pieces = []
        if first > 0:
            pieces.append(jnp.zeros((PAD, first * WIN), f32))
        pieces.extend(rows[n][r * PAD : (r + 1) * PAD] for n in range(count))
        rest = WIDE // WIN - first - count
        pieces.append(jnp.zeros((PAD, rest * WIN), f32))
        line = jnp.concatenate(pieces, axis=1)
        if r > 0:
            line = pltpu.roll(line, PAD * r, axis=1)
        total = line if total is None else total + line
    return total


def gather_back(heads_ref, n, back):
    high = heads_ref[n * GROUP_ROWS : (n + 1) * GROUP_ROWS, :]
    low = heads_ref[heads_ref.shape[0] // 2 + n * GROUP_ROWS : heads_ref.shape[0] // 2 + (n + 1) * GROUP_ROWS, :]
    out = dot(jnp.concatenate([high, low], axis=0), back)
    out = out[:GROUP_ROWS] + out[GROUP_ROWS:]
    return out[:, :WIN] + out[:, WIN:]


def load_flat(dst, src):
    dst[...] = jnp.zeros(dst.shape, f32)
    for i in range(BASIS):
        dst[i : i + 1, : BASIS * BASIS] = src[i]


def element_pairs(groups, ahead, outers, inners, planes, back, weight_ref, base, mid_h, mid_l, prod, heads, hooks=None):
    count = len(groups)
    pairs = 2 * count
    half = heads.shape[0] // 2
    done = []

    def forward(p):
        scale = [weight_ref[:, base + (2 * p + q) * SPAN : base + (2 * p + q + 1) * SPAN] for q in range(2)]
        column = 0
        for outer, sources in zip(outers, planes):
            pieces = []
            for q in range(2):
                row = (2 * p + q) * PAD
                for source in sources:
                    stack = []
                    for block in source:
                        cols = slice(block * SPAN, (block + 1) * SPAN)
                        stack += [mid_h[row : row + PAD, cols], mid_l[row : row + PAD, cols], mid_h[row : row + PAD, cols]]
                    pieces.append(jnp.concatenate(stack, axis=0))
            out = dot(outer, jnp.concatenate(pieces, axis=1))
            wide = jnp.concatenate([scale[q] for q in range(2) for _ in sources], axis=1)
            high, low = split(out * wide)
            width = 2 * len(sources) * SPAN
            prod[p % 2, :QUAD, column : column + width] = high
            prod[p % 2, QUAD:, column : column + width] = low
            column += width

    def backward(p):
        column = 0
        place = 0
        for inner, sources in zip(inners, planes):
            width = 2 * len(sources) * SPAN
            out = dot(inner, prod[p % 2, :, column : column + width])
            high, low = split(out[:PAD] + out[PAD:])
            for q in range(2):
                row = (2 * p + q) * PAD
                take = slice(q * len(sources) * SPAN, (q + 1) * len(sources) * SPAN)
                put = slice(place, place + len(sources) * SPAN)
                heads[row : row + PAD, put] = high[:, take]
                heads[half + row : half + row + PAD, put] = low[:, take]
            column += width
            place += len(sources) * SPAN

    ahead(0)
    for p in range(pairs + 1):
        if p < pairs:
            forward(p)
            if p % 2 == 0 and p // 2 + 1 < count:
                ahead(p // 2 + 1)
        if hooks and p in hooks:
            hooks[p]()
        if p > 0:
            backward(p - 1)
        if p >= 3 and p % 2 == 1:
            done.append(gather_back(heads, len(done), back))
    while len(done) < count:
        done.append(gather_back(heads, len(done), back))
    return overlap(done, groups)


def start_all(pairs, sems):
    copies = [pltpu.make_async_copy(src, dst, sems.at[n]) for n, (src, dst) in enumerate(pairs)]
    for copy in copies:
        copy.start()
    return copies


def stiff_kernel(groups, fetch_lanes, wide_ref, ahead_ref, outer_ref, inner_ref, back_ref, weight_ref, next_hbm, out_ref, next_ref, mid_h, mid_l, prod, heads, sems):
    copies = start_all([(next_hbm.at[0, :, fetch_lanes], next_ref)], sems)
    shifted = shifts(wide_ref[...])

    def ahead(n):
        high, low = split(dot(windows(shifted, groups[n]), ahead_ref[...]))
        mid_h[n * GROUP_ROWS : (n + 1) * GROUP_ROWS, :] = high
        mid_l[n * GROUP_ROWS : (n + 1) * GROUP_ROWS, :] = low

    out_ref[...] = element_pairs(
        groups,
        ahead,
        (outer_ref[0], outer_ref[1]),
        (inner_ref[0], inner_ref[1]),
        (((0,),), ((1,), (2,))),
        back_ref[...],
        weight_ref,
        0,
        mid_h,
        mid_l,
        prod,
        heads,
    )
    for copy in copies:
        copy.wait()


def volume_tables(outer_ref, inner_ref, back_ref):
    sub = lax.axis_index("sub")
    is_pressure = sub == FIELDS - 1
    outer = jnp.concatenate([outer_ref[jnp.where(is_pressure, 0, 1)], outer_ref[1]], axis=1)
    inner = inner_ref[jnp.where(sub == 0, 0, 1)]
    kind = jnp.where(is_pressure, 0, sub)
    back = back_ref[pl.ds(pl.multiple_of(kind * SPAN, SPAN), SPAN), :]
    return outer, inner, back


def volume_groups(groups, wides, ahead_ref, tables, weight_ref, mid_h, mid_l, prod, heads, hooks=None):
    shifted = [shifts(wide) for wide in wides]
    outer, inner, back = tables

    def ahead(n):
        at = slice(n * GROUP_ROWS, (n + 1) * GROUP_ROWS)
        m = groups[n]
        high, low = split(dot(windows(shifted[0], m), ahead_ref[:, :SPAN]))
        mid_h[at, :SPAN] = high
        mid_l[at, :SPAN] = low
        both = jnp.concatenate([windows(shifted[1], m), windows(shifted[2], m)], axis=1)
        high, low = split(dot(both, jnp.concatenate([ahead_ref[:, SPAN : 2 * SPAN], ahead_ref[:, 2 * SPAN :]], axis=0)))
        mid_h[at, SPAN:] = high
        mid_l[at, SPAN:] = low

    base = groups[0] * 4 * SPAN
    return element_pairs(
        groups, ahead, (outer,), (inner,), (((0, 1),),), back, weight_ref, base, mid_h, mid_l, prod, heads, hooks
    )


def volume_kernel(groups, near_ref, far_ref, spread_ref, ahead_ref, outer_ref, inner_ref, back_ref, weight_ref, out_ref, wides_ref, flat, mid_h, mid_l, prod, heads):
    sub = lax.axis_index("sub")
    is_pressure = sub == FIELDS - 1
    load_flat(flat.at[0], near_ref)
    load_flat(flat.at[1], far_ref.at[0])
    load_flat(flat.at[2], far_ref.at[1])
    chosen = jnp.where(is_pressure, 2, 2 - sub)
    zero = jnp.zeros((PAD, FLAT), f32)
    fields = [
        flat[chosen],
        jnp.where(is_pressure, flat[1], zero),
        jnp.where(is_pressure, flat[0], zero),
    ]
    wides = expand(fields, spread_ref[...])
    for n in range(3):
        wides_ref[n] = wides[n]
    tables = volume_tables(outer_ref, inner_ref, back_ref)
    out_ref[...] = volume_groups(groups, wides, ahead_ref, tables, weight_ref, mid_h, mid_l, prod, heads)


def masked(matrix, limit):
    rows = lax.broadcasted_iota(jnp.int32, matrix.shape, 0)
    return jnp.where(rows < limit, matrix, 0.0)


def layers():
    lanes = lax.broadcasted_iota(jnp.int32, (PAD, FLAT), 1)
    group = jnp.floor((lanes.astype(f32) + 0.5) * (1.0 / BASIS)).astype(jnp.int32)
    rows = lax.broadcasted_iota(jnp.int32, (PAD, FLAT), 0)
    inside = lanes - BASIS * group == rows
    return group, rows, jnp.where(inside, 1.0, 0.0).astype(bf16)


def dot_split(a, b, dims):
    a_high, a_low = split(a)
    b_high, b_low = split(b)
    dims = (dims, ((), ()))
    general = functools.partial(lax.dot_general, dimension_numbers=dims, preferred_element_type=f32)
    return general(a_high, b_high) + (general(a_high, b_low) + general(a_low, b_high))


def position(relative, masks):
    total = jnp.int32(0)
    for n, mask in enumerate(masks):
        total = total + jnp.where(jnp.bitwise_and(relative, mask) != 0, jnp.int32(1 << n), jnp.int32(0))
    return total


def routes(links, lines, mine, slots):
    items = 2 * slots
    patch, face = lines[0:2, :], lines[2:4, :]
    hit = jnp.logical_and(patch == mine, jnp.broadcast_to(lines[4:5, :], patch.shape) > 0)
    index = 2 * lax.broadcasted_iota(jnp.int32, patch.shape, 1) + lax.broadcasted_iota(jnp.int32, patch.shape, 0)
    found = [jnp.sum(jnp.where(jnp.logical_and(hit, face == f), index, 0)) for f in range(4)]
    one = lambda flag: jnp.where(flag, jnp.int32(1), jnp.int32(0))
    once = lambda flags: jnp.minimum(functools.reduce(jnp.add, flags, jnp.int32(0)), 1)
    owners = [lax.div(item, items) for item in found]
    faces = []
    for f in range(4):
        mates = [(g, one(owners[g] == owners[f])) for g in range(4) if g != f]
        first = once([mate for g, mate in mates if g < f])
        faces.append((owners[f], first, 2 + once([mate * one(found[g] < found[f]) for g, mate in mates])))
    base = mine * slots
    patch = [links[t % 2, base + t // 2] for t in range(items)]
    alive = [links[4, base + t // 2] > 0 for t in range(items)]
    group = [jnp.where(alive[t], patch[t], -1 - t) for t in range(items)]
    face = [links[2 + t % 2, base + t // 2] for t in range(items)]
    lower = [[] for _ in range(items)]
    earlier = [[] for _ in range(items)]
    for t in range(items):
        for u in range(t):
            same = one(group[u] == group[t])
            below = same * one(face[u] < face[t])
            earlier[t].append(same)
            lower[t].append(below)
            lower[u].append(same - below)
    own = [(patch[t], once(lower[t]), 2 + once(earlier[t])) for t in range(items)]
    return faces, own


def place(block, lane):
    wide = jnp.concatenate([block, jnp.zeros((PAD, WIN - PAD), f32)], axis=1)
    return pltpu.roll(wide, lane * PAD, axis=1)


def prep_kernel(masks, links_hbm, field_hbm, lag_hbm, mortar_hbm, spread_hbm, ahead_hbm, outer_hbm, inner_hbm, back_hbm, weight_hbm, own_ref, wide_ref, sides_ref, route_ref, spread_ref, ahead_ref, outer_ref, inner_ref, back_ref, weight_ref, links, lines, field, lag, mortar, flat, line, sems):
    copies = start_all(
        [
            (field_hbm, field),
            (lag_hbm, lag),
            (links_hbm, links),
            (links_hbm, lines),
            (mortar_hbm, mortar),
            (spread_hbm, spread_ref),
            (ahead_hbm, ahead_ref),
            (outer_hbm, outer_ref),
            (inner_hbm, inner_ref),
            (back_hbm, back_ref),
            (weight_hbm.at[0, :, pl.ds(0, weight_ref.shape[1])], weight_ref),
        ],
        sems,
    )
    slots = lag.shape[0]
    items = 2 * slots
    mine = lax.axis_index("patch")
    own_ref[...] = jnp.zeros(own_ref.shape, f32)
    line[...] = jnp.zeros(line.shape, f32)
    sides_ref[...] = jnp.zeros(sides_ref.shape, f32)
    group, rows, fold = layers()
    same = rows == group
    for copy in copies[:5]:
        copy.wait()
    faces, own = routes(links, lines[...], mine, slots)
    load_flat(flat, field)
    for s in range(slots):
        line[s : s + 1, : BASIS * BASIS] = lag[s, 0]
    spreads = [jnp.where(same, line[s : s + 1, :], 0.0) for s in range(slots)]
    spreads += [
        jnp.where(same, flat[0:1, :], 0.0),
        jnp.where(same, flat[BASIS - 1 : BASIS, :], 0.0),
        jnp.where(group == 0, flat[...], 0.0),
        jnp.where(group == BASIS - 1, flat[...], 0.0),
    ]
    parts = []
    for x in spreads:
        parts.extend(split(x))
    squares = halves_sum(dot_nt(jnp.concatenate(parts, axis=0), fold), 4 + slots)
    base = mine * slots
    for s in range(slots):
        for side in range(2):
            for d in range(2):
                sides_ref[2 * s + side, d, :BASIS, :BASIS] = masked(mortar[s, side, :, d, :], links[4 + d, base + s])
    halfway = [dot_split(sides_ref[t, 0], squares[t // 2], ((0,), (0,))) for t in range(items)]
    copies[5].wait()
    (wide,) = expand([flat[...]], spread_ref[...])
    wide_ref[...] = wide
    for f in range(4):
        patch, first, second = faces[f]
        row = jnp.bitwise_xor(mine, patch)
        own_ref[row] = own_ref[row] + place(squares[slots + f], first)
    for t in range(items):
        both = dot_split(halfway[t], sides_ref[t, 1], ((1,), (0,)))
        patch, first, second = own[t]
        row = jnp.bitwise_xor(mine, patch)
        own_ref[row] = own_ref[row] + place(both if t % 2 == 0 else -both, second)
    entries = []
    for patch, first, second in faces:
        entries += [position(jnp.bitwise_xor(mine, patch), masks), second]
    for patch, first, second in own:
        entries += [position(jnp.bitwise_xor(mine, patch), masks), first]
    lane = lax.broadcasted_iota(jnp.int32, route_ref.shape, 1)
    table = jnp.zeros(route_ref.shape, jnp.int32)
    for n, entry in enumerate(entries):
        table = jnp.where(lane == n, entry, table)
    route_ref[...] = table
    for copy in copies[6:]:
        copy.wait()


def final_kernel(groups, route_vmem, sides_ref, kept_ref, other_ref, stiff_a, stiff_b, volume_ref, wides_ref, spread_ref, ahead_ref, outer_ref, inner_ref, back_ref, weight_ref, out_ref, jump_ref, buf, mid_h, mid_l, prod, heads, route, sems):
    copies = start_all([(route_vmem, route)], sems)
    items = sides_ref.shape[0]
    slots = items // 2
    half = kept_ref.shape[0]
    buf[:half] = kept_ref[...]
    buf[half:] = other_ref[...]
    group, rows, fold = layers()
    same = rows == group
    squares = []
    halfway = []
    both = []

    def pick(n):
        block = buf[route[0, 2 * n]]
        return pltpu.roll(block, lax.rem(WIN - route[0, 2 * n + 1] * PAD, WIN), axis=1)[:, :PAD]

    def start():
        copies[0].wait()
        halfway.extend(dot_split(sides_ref[t, 0], pick(4 + t), ((1,), (0,))) for t in range(items))
        squares.extend(pick(f) for f in range(4))

    def go_on():
        both.extend(dot_split(halfway[t], sides_ref[t, 1], ((1,), (1,))) for t in range(items))

    def end():
        for s in range(slots):
            squares.append(both[2 * s] - both[2 * s + 1])
        parts = []
        for x in squares:
            parts.extend(split(x))
        lines = halves_sum(dot(jnp.concatenate(parts, axis=0), fold), 4 + slots)
        for s in range(slots):
            row = jnp.sum(jnp.where(same, lines[4 + s], 0.0), axis=0, keepdims=True)
            jump_ref[s, 0] = row[:, : BASIS * BASIS]
        low_row = jnp.sum(jnp.where(same, lines[0], 0.0), axis=0, keepdims=True)
        high_row = jnp.sum(jnp.where(same, lines[1], 0.0), axis=0, keepdims=True)
        both.append(
            jnp.where(rows == 0, low_row, 0.0)
            + jnp.where(rows == BASIS - 1, high_row, 0.0)
            + jnp.where(group == 0, lines[2], 0.0)
            + jnp.where(group == BASIS - 1, lines[3], 0.0)
        )

    tables = volume_tables(outer_ref, inner_ref, back_ref)
    volume = volume_groups(
        groups,
        [wides_ref[n] for n in range(3)],
        ahead_ref,
        tables,
        weight_ref,
        mid_h,
        mid_l,
        prod,
        heads,
        {0: start, 1: go_on, 2: end},
    )
    is_pressure = lax.axis_index("sub") == FIELDS - 1
    factor = jnp.where(is_pressure, -stabilize, 1.0).astype(f32)
    total = factor * (stiff_a[...] + stiff_b[...]) - (volume_ref[...] + volume)
    out = dot_nt(jnp.concatenate(split(total), axis=0), spread_ref[...])
    out = out[:PAD] + out[PAD:] + both[-1]
    for i in range(BASIS):
        out_ref[i] = out[i : i + 1, : BASIS * BASIS]


def vmem():
    return pl.BlockSpec(memory_space=pltpu.VMEM)


def anywhere():
    return pl.BlockSpec(memory_space=pltpu.HBM)


def in_hbm(*arrays):
    return [pltpu.with_memory_space_constraint(x, pltpu.HBM) for x in arrays]


params = pltpu.CompilerParams(vmem_limit_bytes=24 << 20)
halfspan = (GROUPS // 2) * 4 * SPAN


def stiff_call(groups, fetch, wide, tables, weight, following):
    count = 4 * len(groups)
    lanes = pl.ds(fetch[0], fetch[1])
    return pl.pallas_call(
        functools.partial(stiff_kernel, groups, lanes),
        out_shape=(
            jax.ShapeDtypeStruct((PAD, WIDE), f32),
            jax.ShapeDtypeStruct((QUAD, fetch[1]), f32),
        ),
        in_specs=[vmem()] * 6 + [anywhere()],
        out_specs=(vmem(), vmem()),
        scratch_shapes=[
            pltpu.VMEM((count * PAD, 3 * SPAN), bf16),
            pltpu.VMEM((count * PAD, 3 * SPAN), bf16),
            pltpu.VMEM((2, 2 * QUAD, 6 * SPAN), bf16),
            pltpu.VMEM((2 * count * PAD, 3 * SPAN), bf16),
            pltpu.SemaphoreType.DMA((1,)),
        ],
        compiler_params=params,
    )(wide, *tables[1:], weight, *in_hbm(following))


def volume_scratch(count):
    return [
        pltpu.VMEM((count * GROUP_ROWS, 2 * SPAN), bf16),
        pltpu.VMEM((count * GROUP_ROWS, 2 * SPAN), bf16),
        pltpu.VMEM((2, 2 * QUAD, 2 * SPAN), bf16),
        pltpu.VMEM((2 * count * GROUP_ROWS, SPAN), bf16),
    ]


def volume_call(groups, near, far, tables, weight):
    return pl.pallas_call(
        functools.partial(volume_kernel, groups),
        out_shape=(jax.ShapeDtypeStruct((PAD, WIDE), f32), jax.ShapeDtypeStruct((3, PAD, WIDE), f32)),
        in_specs=[vmem()] * 8,
        out_specs=(vmem(), vmem()),
        scratch_shapes=[pltpu.VMEM((3, PAD, FLAT), f32)] + volume_scratch(len(groups)),
        compiler_params=params,
    )(near, far, *tables, weight)


def prep_call(masks, links, field, lagrange, mortar, tables, stiff_weight):
    slots = mortar.shape[0]
    patches = 1 << len(masks)
    return pl.pallas_call(
        functools.partial(prep_kernel, masks),
        out_shape=(
            jax.ShapeDtypeStruct((patches, PAD, WIN), f32),
            jax.ShapeDtypeStruct((PAD, WIDE), f32),
            jax.ShapeDtypeStruct((2 * slots, 2, PAD, PAD), f32),
            jax.ShapeDtypeStruct((1, WIN), jnp.int32),
            *(jax.ShapeDtypeStruct(t.shape, bf16) for t in tables),
            jax.ShapeDtypeStruct((QUAD, halfspan), f32),
        ),
        in_specs=[anywhere()] * 10,
        out_specs=(vmem(),) * 10,
        scratch_shapes=[
            pltpu.SMEM(links.shape, jnp.int32),
            pltpu.VMEM(links.shape, jnp.int32),
            pltpu.VMEM(field.shape, f32),
            pltpu.VMEM(lagrange.shape, f32),
            pltpu.VMEM(mortar.shape, f32),
            pltpu.VMEM((PAD, FLAT), f32),
            pltpu.VMEM((8, FLAT), f32),
            pltpu.SemaphoreType.DMA((11,)),
        ],
        compiler_params=params,
    )(*in_hbm(links, field, lagrange, mortar, *tables, stiff_weight))


def final_call(groups, route, sides, kept, other, stiff_a, stiff_b, volume, wides, tables, weight, field):
    slots = sides.shape[0] // 2
    return pl.pallas_call(
        functools.partial(final_kernel, groups),
        out_shape=(
            jax.ShapeDtypeStruct(field.shape, f32),
            jax.ShapeDtypeStruct((slots, 1, 1, BASIS * BASIS), f32),
        ),
        in_specs=[vmem()] * 14,
        out_specs=(vmem(), vmem()),
        scratch_shapes=[pltpu.VMEM((2 * kept.shape[0], PAD, WIN), f32)]
        + volume_scratch(len(groups))
        + [pltpu.SMEM((1, WIN), jnp.int32), pltpu.SemaphoreType.DMA((1,))],
        compiler_params=params,
    )(route, sides, kept, other, stiff_a, stiff_b, volume, wides, *tables, weight)


def swap(array, axis, mask):
    size = lax.axis_size(axis)
    return lax.ppermute(array, axis, [(n, n ^ mask) for n in range(size)])


def after(array, *others):
    return lax.optimization_barrier((array,) + others)[0]


def per_device(state, stiff_weight, volume_weight, lagrange, mortar, links):
    tables = [jnp.asarray(constants()[name]) for name in ("spread", "ahead", "outer", "inner", "back")]
    patches = lax.axis_size("patch")
    masks = [1 << n for n in reversed(range(patches.bit_length() - 1))]
    field = jnp.transpose(state, (0, 1, 3, 2, 4))[0, 0]
    mortar = jnp.transpose(mortar, (0, 1, 3, 2, 4))
    links = links.T

    near = swap(field, "sub", 1)
    own, wide, sides, route, *tables, weight_a = prep_call(masks, links, field, lagrange, mortar, tables, stiff_weight)
    far = swap(jnp.stack([field, near]), "sub", 2)
    first = GROUPS // 2
    stiff_a, weight_b = stiff_call(
        list(range(first)), (halfspan, ELEMS * SPAN - halfspan), wide, tables, weight_a, stiff_weight
    )
    stiff_b, weight_c = stiff_call(list(range(first, GROUPS)), (0, ELEMS * SPAN), wide, tables, weight_b, volume_weight)
    volume, wides = volume_call(list(range(EARLY)), near, far, tables, weight_c)
    gates = [None, stiff_a, stiff_b]
    held = own[None]
    for n, mask in enumerate(masks):
        late = len(masks) - n
        gate = gates[max(0, 3 - late)]
        half = held.shape[1] // 2
        send = held[:, half:]
        other = swap(send if gate is None else after(send, gate), "patch", mask)
        kept = held[:, :half]
        held = jnp.concatenate([kept, other], axis=0)
    residual, constraint = final_call(
        list(range(EARLY, GROUPS)), route, sides, kept[:, 0], other[:, 0], stiff_a, stiff_b, volume, wides, tables, weight_c, field
    )
    return jnp.transpose(residual[None, None], (0, 1, 3, 2, 4)), constraint


def solution(mesh):
    return jax.shard_map(
        per_device,
        mesh=mesh,
        in_specs=(
            P("patch", "sub", None, None, None),
            P("patch", None, None),
            P("patch", None, None),
            P("patch", "sub", None, None),
            P("patch", None, None, None, None),
            P(),
        ),
        out_specs=(P("patch", "sub", None, None, None), P("patch", "sub", None, None)),
        check_vma=False,
    )
```

```python
import functools

import jax
import jax.numpy as jnp
import numpy as np
from jax import lax
from jax.experimental import pallas as pl
from jax.experimental.pallas import tpu as pltpu
from jax.sharding import PartitionSpec as P


ELEMS = 24
DEGREE = 3
FIELDS = 4
LOCAL = DEGREE + 1
NODES = 4
BASIS = ELEMS + DEGREE
QUAD = ELEMS * NODES
PAD = 32
WIN = LOCAL * PAD
SPAN = NODES * QUAD
GROUPS = ELEMS // 4
EARLY = GROUPS - 2
WIDE = (GROUPS + 1) * WIN
FLAT = 768
GROUP_ROWS = 4 * PAD
BLOCK = 256
BLOCK_WIDE = 384

stabilize = 0.25
f32 = jnp.float32
bf16 = jnp.bfloat16
gauss_points_four = [
    -0.8611363115940526,
    -0.3399810435848563,
    0.3399810435848563,
    0.8611363115940526,
]
gauss_weights_four = [
    0.3478548451374538,
    0.6521451548625461,
    0.6521451548625461,
    0.3478548451374538,
]


def spline_tables(knot_list, points, degree):
    current = np.where(
        (knot_list[None, :-1] <= points[:, None]) & (points[:, None] < knot_list[None, 1:]),
        1.0,
        0.0,
    )
    previous = current
    for order_k in range(1, degree + 1):
        previous = current
        amount = len(knot_list) - 1 - order_k
        current = np.zeros((points.shape[0], amount))
        for column in range(amount):
            left_span = knot_list[column + order_k] - knot_list[column]
            right_span = knot_list[column + order_k + 1] - knot_list[column + 1]
            if left_span > 0:
                current[:, column] += (points - knot_list[column]) / left_span * previous[:, column]
            if right_span > 0:
                current[:, column] += (
                    (knot_list[column + order_k + 1] - points)
                    / right_span
                    * previous[:, column + 1]
                )
    slope_part = np.zeros(current.shape)
    for column in range(current.shape[1]):
        left_span = knot_list[column + degree] - knot_list[column]
        right_span = knot_list[column + degree + 1] - knot_list[column + 1]
        if left_span > 0:
            slope_part[:, column] += degree / left_span * previous[:, column]
        if right_span > 0:
            slope_part[:, column] -= degree / right_span * previous[:, column + 1]
    return current, slope_part


def halves(table):
    high = table.astype(np.dtype(bf16)).astype(np.float64)
    return high, table - high


def padded(table, rows, cols):
    out = np.zeros((rows, cols))
    out[: table.shape[0], : table.shape[1]] = table
    return out


@functools.cache
def constants():
    nodes = np.array(gauss_points_four)
    points = (np.arange(ELEMS)[:, None] + (nodes[None, :] + 1.0) / 2.0).reshape(-1)
    weights = np.tile(np.array(gauss_weights_four) / 2.0, ELEMS)
    open_knots = np.concatenate(
        [np.zeros(DEGREE), np.arange(ELEMS + 1.0), np.full(DEGREE, float(ELEMS))]
    )
    even_knots = np.arange(-DEGREE, ELEMS + DEGREE + 1.0)
    value, slope = spline_tables(open_knots, points, DEGREE)
    even_value, even_slope = spline_tables(even_knots, points, DEGREE)
    change = np.round(np.linalg.lstsq(even_value, value, rcond=None)[0] * 4.0) / 4.0
    local_value = even_value[4 * NODES : 5 * NODES, 4 : 4 + LOCAL]
    local_slope = even_slope[4 * NODES : 5 * NODES, 4 : 4 + LOCAL]
    local_w = weights[:NODES, None]

    def kron(local, table):
        wide = padded(table, QUAD, PAD)
        return np.einsum("bj,ck->jkbc", local, wide).reshape(WIN, SPAN)

    ahead = np.concatenate(
        [kron(local_value, value), kron(local_slope, value), kron(local_value, slope)], axis=1
    )
    value_w, slope_w = value * weights[:, None], slope * weights[:, None]
    back = np.concatenate(
        [
            kron(local_value * local_w, value_w).T,
            kron(local_slope * local_w, value_w).T,
            kron(local_value * local_w, slope_w).T,
        ],
        axis=0,
    )
    ahead_high, ahead_low = halves(ahead)
    ahead3 = np.concatenate([ahead_high, ahead_high, ahead_low], axis=0)
    back_high, back_low = halves(back)
    back2 = np.concatenate([back_high, back_low], axis=1)

    def left3(table):
        high, low = halves(padded(table, QUAD, PAD))
        return np.concatenate([high, high, low], axis=1)

    def left4(table):
        high, low = halves(padded(table, QUAD, PAD).T)
        return np.concatenate(
            [np.concatenate([high, high], axis=1), np.concatenate([low, low], axis=1)], axis=0
        )

    spread = np.zeros((BASIS, BASIS, WIDE // PAD, PAD))
    for k in range(BASIS):
        spread[:, k, :BASIS, k] = change.T
    spread = padded(spread.reshape(BASIS * BASIS, WIDE), FLAT, WIDE)
    blocks = [
        spread[n * BLOCK : (n + 1) * BLOCK, n * BLOCK : n * BLOCK + BLOCK_WIDE] for n in range(FLAT // BLOCK)
    ]
    assert sum(np.count_nonzero(block) for block in blocks) == np.count_nonzero(spread)
    as16 = lambda a: a.astype(np.dtype(bf16))
    return dict(
        ahead=as16(ahead3),
        back=as16(back2),
        outer=as16(np.stack([left3(slope), left3(value)])),
        inner=as16(np.stack([left4(slope_w), left4(value_w)])),
        spread=as16(np.stack(blocks)),
    )


def split(x):
    high = x.astype(bf16)
    return high, (x - high.astype(f32)).astype(bf16)


def dot(a, b):
    return jnp.dot(a, b, preferred_element_type=f32)


def dot_nt(a, b):
    return lax.dot_general(a, b, (((1,), (1,)), ((), ())), preferred_element_type=f32)


def expand(fields, spread_ref):
    parts = []
    for field in fields:
        parts.extend(split(field))
    rows = jnp.concatenate(parts, axis=0)
    out = None
    for n in range(FLAT // BLOCK):
        piece = dot(rows[:, n * BLOCK : (n + 1) * BLOCK], spread_ref[n])
        left, right = n * BLOCK, WIDE - n * BLOCK - BLOCK_WIDE
        sides = [jnp.zeros((rows.shape[0], width), f32) for width in (left, right)]
        pieces = ([sides[0]] if left else []) + [piece] + ([sides[1]] if right else [])
        piece = jnp.concatenate(pieces, axis=1)
        out = piece if out is None else out + piece
    return halves_sum(out, len(fields))


def contract(wide, spread_ref):
    rows = jnp.concatenate(split(wide), axis=0)
    out = [
        dot_nt(rows[:, n * BLOCK : n * BLOCK + BLOCK_WIDE], spread_ref[n]) for n in range(FLAT // BLOCK)
    ]
    return halves_sum(jnp.concatenate(out, axis=1), 1)[0]


def halves_sum(out, count):
    return [
        out[2 * n * PAD : (2 * n + 1) * PAD] + out[(2 * n + 1) * PAD : (2 * n + 2) * PAD]
        for n in range(count)
    ]


def shifts(wide):
    rolled = [wide] + [pltpu.roll(wide, WIDE - PAD * r, axis=1) for r in range(1, 4)]
    return [split(x) for x in rolled]


def windows(shifted, m):
    rows = []
    for r in range(4):
        high = shifted[r][0][:, m * WIN : (m + 1) * WIN]
        low = shifted[r][1][:, m * WIN : (m + 1) * WIN]
        rows.append(jnp.concatenate([high, low, high], axis=1))
    return jnp.concatenate(rows, axis=0)


def overlap(rows, groups):
    first, count = groups[0], len(groups)
    total = None
    for r in range(4):
        pieces = []
        if first > 0:
            pieces.append(jnp.zeros((PAD, first * WIN), f32))
        pieces.extend(rows[n][r * PAD : (r + 1) * PAD] for n in range(count))
        rest = WIDE // WIN - first - count
        pieces.append(jnp.zeros((PAD, rest * WIN), f32))
        line = jnp.concatenate(pieces, axis=1)
        if r > 0:
            line = pltpu.roll(line, PAD * r, axis=1)
        total = line if total is None else total + line
    return total


def gather_back(heads_ref, n, back):
    high = heads_ref[n * GROUP_ROWS : (n + 1) * GROUP_ROWS, :]
    low = heads_ref[heads_ref.shape[0] // 2 + n * GROUP_ROWS : heads_ref.shape[0] // 2 + (n + 1) * GROUP_ROWS, :]
    out = dot(jnp.concatenate([high, low], axis=0), back)
    out = out[:GROUP_ROWS] + out[GROUP_ROWS:]
    return out[:, :WIN] + out[:, WIN:]


def load_flat(dst, src):
    dst[...] = jnp.zeros(dst.shape, f32)
    for i in range(BASIS):
        dst[i : i + 1, : BASIS * BASIS] = src[i]


def element_pairs(groups, ahead, outers, inners, planes, back, weight_ref, base, mid_h, mid_l, prod, heads, hooks=None):
    count = len(groups)
    pairs = 2 * count
    half = heads.shape[0] // 2
    done = []

    def forward(p):
        scale = [weight_ref[:, base + (2 * p + q) * SPAN : base + (2 * p + q + 1) * SPAN] for q in range(2)]
        column = 0
        for outer, sources in zip(outers, planes):
            pieces = []
            for q in range(2):
                row = (2 * p + q) * PAD
                for source in sources:
                    stack = []
                    for block in source:
                        cols = slice(block * SPAN, (block + 1) * SPAN)
                        stack += [mid_h[row : row + PAD, cols], mid_l[row : row + PAD, cols], mid_h[row : row + PAD, cols]]
                    pieces.append(jnp.concatenate(stack, axis=0))
            out = dot(outer, jnp.concatenate(pieces, axis=1))
            wide = jnp.concatenate([scale[q] for q in range(2) for _ in sources], axis=1)
            high, low = split(out * wide)
            width = 2 * len(sources) * SPAN
            prod[p % 2, :QUAD, column : column + width] = high
            prod[p % 2, QUAD:, column : column + width] = low
            column += width

    def backward(p):
        column = 0
        place = 0
        for inner, sources in zip(inners, planes):
            width = 2 * len(sources) * SPAN
            out = dot(inner, prod[p % 2, :, column : column + width])
            high, low = split(out[:PAD] + out[PAD:])
            for q in range(2):
                row = (2 * p + q) * PAD
                take = slice(q * len(sources) * SPAN, (q + 1) * len(sources) * SPAN)
                put = slice(place, place + len(sources) * SPAN)
                heads[row : row + PAD, put] = high[:, take]
                heads[half + row : half + row + PAD, put] = low[:, take]
            column += width
            place += len(sources) * SPAN

    ahead(0)
    for p in range(pairs + 1):
        if p < pairs:
            forward(p)
            if p % 2 == 0 and p // 2 + 1 < count:
                ahead(p // 2 + 1)
        if hooks and p in hooks:
            hooks[p]()
        if p > 0:
            backward(p - 1)
        if p >= 3 and p % 2 == 1:
            done.append(gather_back(heads, len(done), back))
    while len(done) < count:
        done.append(gather_back(heads, len(done), back))
    return overlap(done, groups)


def start_all(pairs, sems):
    copies = [pltpu.make_async_copy(src, dst, sems.at[n]) for n, (src, dst) in enumerate(pairs)]
    for copy in copies:
        copy.start()
    return copies


def stiff_kernel(groups, fetch_lanes, wide_ref, ahead_ref, outer_ref, inner_ref, back_ref, weight_ref, next_hbm, out_ref, next_ref, mid_h, mid_l, prod, heads, sems):
    copies = start_all([(next_hbm.at[0, :, fetch_lanes], next_ref)], sems)
    shifted = shifts(wide_ref[...])

    def ahead(n):
        high, low = split(dot(windows(shifted, groups[n]), ahead_ref[...]))
        mid_h[n * GROUP_ROWS : (n + 1) * GROUP_ROWS, :] = high
        mid_l[n * GROUP_ROWS : (n + 1) * GROUP_ROWS, :] = low

    out_ref[...] = element_pairs(
        groups,
        ahead,
        (outer_ref[0], outer_ref[1]),
        (inner_ref[0], inner_ref[1]),
        (((0,),), ((1,), (2,))),
        back_ref[...],
        weight_ref,
        0,
        mid_h,
        mid_l,
        prod,
        heads,
    )
    for copy in copies:
        copy.wait()


def volume_tables(outer_ref, inner_ref, back_ref):
    sub = lax.axis_index("sub")
    is_pressure = sub == FIELDS - 1
    outer = jnp.concatenate([outer_ref[jnp.where(is_pressure, 0, 1)], outer_ref[1]], axis=1)
    inner = inner_ref[jnp.where(sub == 0, 0, 1)]
    kind = jnp.where(is_pressure, 0, sub)
    back = back_ref[pl.ds(pl.multiple_of(kind * SPAN, SPAN), SPAN), :]
    return outer, inner, back


def volume_groups(groups, wides, ahead_ref, tables, weight_ref, mid_h, mid_l, prod, heads, hooks=None):
    shifted = [shifts(wide) for wide in wides]
    outer, inner, back = tables

    def ahead(n):
        at = slice(n * GROUP_ROWS, (n + 1) * GROUP_ROWS)
        m = groups[n]
        high, low = split(dot(windows(shifted[0], m), ahead_ref[:, :SPAN]))
        mid_h[at, :SPAN] = high
        mid_l[at, :SPAN] = low
        both = jnp.concatenate([windows(shifted[1], m), windows(shifted[2], m)], axis=1)
        high, low = split(dot(both, jnp.concatenate([ahead_ref[:, SPAN : 2 * SPAN], ahead_ref[:, 2 * SPAN :]], axis=0)))
        mid_h[at, SPAN:] = high
        mid_l[at, SPAN:] = low

    base = groups[0] * 4 * SPAN
    return element_pairs(
        groups, ahead, (outer,), (inner,), (((0, 1),),), back, weight_ref, base, mid_h, mid_l, prod, heads, hooks
    )


def volume_kernel(groups, near_ref, far_ref, spread_ref, ahead_ref, outer_ref, inner_ref, back_ref, weight_ref, out_ref, wides_ref, flat, mid_h, mid_l, prod, heads):
    sub = lax.axis_index("sub")
    is_pressure = sub == FIELDS - 1
    load_flat(flat.at[0], near_ref)
    load_flat(flat.at[1], far_ref.at[0])
    load_flat(flat.at[2], far_ref.at[1])
    chosen = jnp.where(is_pressure, 2, 2 - sub)
    zero = jnp.zeros((PAD, FLAT), f32)
    fields = [
        flat[chosen],
        jnp.where(is_pressure, flat[1], zero),
        jnp.where(is_pressure, flat[0], zero),
    ]
    wides = expand(fields, spread_ref)
    for n in range(3):
        wides_ref[n] = wides[n]
    tables = volume_tables(outer_ref, inner_ref, back_ref)
    out_ref[...] = volume_groups(groups, wides, ahead_ref, tables, weight_ref, mid_h, mid_l, prod, heads)


def masked(matrix, limit):
    rows = lax.broadcasted_iota(jnp.int32, matrix.shape, 0)
    return jnp.where(rows < limit, matrix, 0.0)


def layers():
    lanes = lax.broadcasted_iota(jnp.int32, (PAD, FLAT), 1)
    group = jnp.floor((lanes.astype(f32) + 0.5) * (1.0 / BASIS)).astype(jnp.int32)
    rows = lax.broadcasted_iota(jnp.int32, (PAD, FLAT), 0)
    inside = lanes - BASIS * group == rows
    return group, rows, jnp.where(inside, 1.0, 0.0).astype(bf16)


def dot_split(a, b, dims):
    a_high, a_low = split(a)
    b_high, b_low = split(b)
    dims = (dims, ((), ()))
    general = functools.partial(lax.dot_general, dimension_numbers=dims, preferred_element_type=f32)
    return general(a_high, b_high) + (general(a_high, b_low) + general(a_low, b_high))


def position(relative, masks):
    total = jnp.int32(0)
    for n, mask in enumerate(masks):
        total = total + jnp.where(jnp.bitwise_and(relative, mask) != 0, jnp.int32(1 << n), jnp.int32(0))
    return total


def routes(links, lines, mine, slots):
    items = 2 * slots
    patch, face = lines[0:2, :], lines[2:4, :]
    hit = jnp.logical_and(patch == mine, jnp.broadcast_to(lines[4:5, :], patch.shape) > 0)
    index = 2 * lax.broadcasted_iota(jnp.int32, patch.shape, 1) + lax.broadcasted_iota(jnp.int32, patch.shape, 0)
    found = [jnp.sum(jnp.where(jnp.logical_and(hit, face == f), index, 0)) for f in range(4)]
    one = lambda flag: jnp.where(flag, jnp.int32(1), jnp.int32(0))
    once = lambda flags: jnp.minimum(functools.reduce(jnp.add, flags, jnp.int32(0)), 1)
    owners = [lax.div(item, items) for item in found]
    faces = []
    for f in range(4):
        mates = [(g, one(owners[g] == owners[f])) for g in range(4) if g != f]
        first = once([mate for g, mate in mates if g < f])
        faces.append((owners[f], first, 2 + once([mate * one(found[g] < found[f]) for g, mate in mates])))
    base = mine * slots
    patch = [links[t % 2, base + t // 2] for t in range(items)]
    alive = [links[4, base + t // 2] > 0 for t in range(items)]
    group = [jnp.where(alive[t], patch[t], -1 - t) for t in range(items)]
    face = [links[2 + t % 2, base + t // 2] for t in range(items)]
    lower = [[] for _ in range(items)]
    earlier = [[] for _ in range(items)]
    for t in range(items):
        for u in range(t):
            same = one(group[u] == group[t])
            below = same * one(face[u] < face[t])
            earlier[t].append(same)
            lower[t].append(below)
            lower[u].append(same - below)
    own = [(patch[t], once(lower[t]), 2 + once(earlier[t])) for t in range(items)]
    return faces, own


def place(block, lane):
    wide = jnp.concatenate([block, jnp.zeros((PAD, WIN - PAD), f32)], axis=1)
    return pltpu.roll(wide, lane * PAD, axis=1)


def prep_kernel(masks, links_hbm, field_hbm, lag_hbm, mortar_hbm, spread_hbm, ahead_hbm, outer_hbm, inner_hbm, back_hbm, weight_hbm, own_ref, wide_ref, sides_ref, route_ref, spread_ref, ahead_ref, outer_ref, inner_ref, back_ref, weight_ref, links, lines, field, lag, mortar, flat, line, sems):
    copies = start_all(
        [
            (field_hbm, field),
            (lag_hbm, lag),
            (links_hbm, links),
            (links_hbm, lines),
            (mortar_hbm, mortar),
            (spread_hbm, spread_ref),
            (ahead_hbm, ahead_ref),
            (outer_hbm, outer_ref),
            (inner_hbm, inner_ref),
            (back_hbm, back_ref),
            (weight_hbm.at[0, :, pl.ds(0, weight_ref.shape[1])], weight_ref),
        ],
        sems,
    )
    slots = lag.shape[0]
    items = 2 * slots
    mine = lax.axis_index("patch")
    own_ref[...] = jnp.zeros(own_ref.shape, f32)
    line[...] = jnp.zeros(line.shape, f32)
    sides_ref[...] = jnp.zeros(sides_ref.shape, f32)
    group, rows, fold = layers()
    same = rows == group
    for copy in copies[:5]:
        copy.wait()
    faces, own = routes(links, lines[...], mine, slots)
    load_flat(flat, field)
    for s in range(slots):
        line[s : s + 1, : BASIS * BASIS] = lag[s, 0]
    spreads = [jnp.where(same, line[s : s + 1, :], 0.0) for s in range(slots)]
    spreads += [
        jnp.where(same, flat[0:1, :], 0.0),
        jnp.where(same, flat[BASIS - 1 : BASIS, :], 0.0),
        jnp.where(group == 0, flat[...], 0.0),
        jnp.where(group == BASIS - 1, flat[...], 0.0),
    ]
    parts = []
    for x in spreads:
        parts.extend(split(x))
    squares = halves_sum(dot_nt(jnp.concatenate(parts, axis=0), fold), 4 + slots)
    base = mine * slots
    for s in range(slots):
        for side in range(2):
            for d in range(2):
                sides_ref[2 * s + side, d, :BASIS, :BASIS] = masked(mortar[s, side, :, d, :], links[4 + d, base + s])
    halfway = [dot_split(sides_ref[t, 0], squares[t // 2], ((0,), (0,))) for t in range(items)]
    copies[5].wait()
    (wide,) = expand([flat[...]], spread_ref)
    wide_ref[...] = wide
    for f in range(4):
        patch, first, second = faces[f]
        row = jnp.bitwise_xor(mine, patch)
        own_ref[row] = own_ref[row] + place(squares[slots + f], first)
    for t in range(items):
        both = dot_split(halfway[t], sides_ref[t, 1], ((1,), (0,)))
        patch, first, second = own[t]
        row = jnp.bitwise_xor(mine, patch)
        own_ref[row] = own_ref[row] + place(both if t % 2 == 0 else -both, second)
    entries = []
    for patch, first, second in faces:
        entries += [position(jnp.bitwise_xor(mine, patch), masks), second]
    for patch, first, second in own:
        entries += [position(jnp.bitwise_xor(mine, patch), masks), first]
    lane = lax.broadcasted_iota(jnp.int32, route_ref.shape, 1)
    table = jnp.zeros(route_ref.shape, jnp.int32)
    for n, entry in enumerate(entries):
        table = jnp.where(lane == n, entry, table)
    route_ref[...] = table
    for copy in copies[6:]:
        copy.wait()


def final_kernel(groups, route_vmem, sides_ref, kept_ref, other_ref, stiff_a, stiff_b, volume_ref, wides_ref, spread_ref, ahead_ref, outer_ref, inner_ref, back_ref, weight_ref, out_ref, jump_ref, buf, mid_h, mid_l, prod, heads, route, sems):
    copies = start_all([(route_vmem, route)], sems)
    items = sides_ref.shape[0]
    slots = items // 2
    half = kept_ref.shape[0]
    buf[:half] = kept_ref[...]
    buf[half:] = other_ref[...]
    group, rows, fold = layers()
    same = rows == group
    squares = []
    halfway = []
    both = []

    def pick(n):
        block = buf[route[0, 2 * n]]
        return pltpu.roll(block, lax.rem(WIN - route[0, 2 * n + 1] * PAD, WIN), axis=1)[:, :PAD]

    def start():
        copies[0].wait()
        halfway.extend(dot_split(sides_ref[t, 0], pick(4 + t), ((1,), (0,))) for t in range(items))
        squares.extend(pick(f) for f in range(4))

    def go_on():
        both.extend(dot_split(halfway[t], sides_ref[t, 1], ((1,), (1,))) for t in range(items))

    def end():
        for s in range(slots):
            squares.append(both[2 * s] - both[2 * s + 1])
        parts = []
        for x in squares:
            parts.extend(split(x))
        lines = halves_sum(dot(jnp.concatenate(parts, axis=0), fold), 4 + slots)
        for s in range(slots):
            row = jnp.sum(jnp.where(same, lines[4 + s], 0.0), axis=0, keepdims=True)
            jump_ref[s, 0] = row[:, : BASIS * BASIS]
        low_row = jnp.sum(jnp.where(same, lines[0], 0.0), axis=0, keepdims=True)
        high_row = jnp.sum(jnp.where(same, lines[1], 0.0), axis=0, keepdims=True)
        both.append(
            jnp.where(rows == 0, low_row, 0.0)
            + jnp.where(rows == BASIS - 1, high_row, 0.0)
            + jnp.where(group == 0, lines[2], 0.0)
            + jnp.where(group == BASIS - 1, lines[3], 0.0)
        )

    tables = volume_tables(outer_ref, inner_ref, back_ref)
    volume = volume_groups(
        groups,
        [wides_ref[n] for n in range(3)],
        ahead_ref,
        tables,
        weight_ref,
        mid_h,
        mid_l,
        prod,
        heads,
        {0: start, 1: go_on, 2: end},
    )
    is_pressure = lax.axis_index("sub") == FIELDS - 1
    factor = jnp.where(is_pressure, -stabilize, 1.0).astype(f32)
    total = factor * (stiff_a[...] + stiff_b[...]) - (volume_ref[...] + volume)
    out = contract(total, spread_ref) + both[-1]
    for i in range(BASIS):
        out_ref[i] = out[i : i + 1, : BASIS * BASIS]


def vmem():
    return pl.BlockSpec(memory_space=pltpu.VMEM)


def anywhere():
    return pl.BlockSpec(memory_space=pltpu.HBM)


def in_hbm(*arrays):
    return [pltpu.with_memory_space_constraint(x, pltpu.HBM) for x in arrays]


params = pltpu.CompilerParams(vmem_limit_bytes=24 << 20)
halfspan = (GROUPS // 2) * 4 * SPAN


def stiff_call(groups, fetch, wide, tables, weight, following):
    count = 4 * len(groups)
    lanes = pl.ds(fetch[0], fetch[1])
    return pl.pallas_call(
        functools.partial(stiff_kernel, groups, lanes),
        out_shape=(
            jax.ShapeDtypeStruct((PAD, WIDE), f32),
            jax.ShapeDtypeStruct((QUAD, fetch[1]), f32),
        ),
        in_specs=[vmem()] * 6 + [anywhere()],
        out_specs=(vmem(), vmem()),
        scratch_shapes=[
            pltpu.VMEM((count * PAD, 3 * SPAN), bf16),
            pltpu.VMEM((count * PAD, 3 * SPAN), bf16),
            pltpu.VMEM((2, 2 * QUAD, 6 * SPAN), bf16),
            pltpu.VMEM((2 * count * PAD, 3 * SPAN), bf16),
            pltpu.SemaphoreType.DMA((1,)),
        ],
        compiler_params=params,
    )(wide, *tables[1:], weight, *in_hbm(following))


def volume_scratch(count):
    return [
        pltpu.VMEM((count * GROUP_ROWS, 2 * SPAN), bf16),
        pltpu.VMEM((count * GROUP_ROWS, 2 * SPAN), bf16),
        pltpu.VMEM((2, 2 * QUAD, 2 * SPAN), bf16),
        pltpu.VMEM((2 * count * GROUP_ROWS, SPAN), bf16),
    ]


def volume_call(groups, near, far, tables, weight):
    return pl.pallas_call(
        functools.partial(volume_kernel, groups),
        out_shape=(jax.ShapeDtypeStruct((PAD, WIDE), f32), jax.ShapeDtypeStruct((3, PAD, WIDE), f32)),
        in_specs=[vmem()] * 8,
        out_specs=(vmem(), vmem()),
        scratch_shapes=[pltpu.VMEM((3, PAD, FLAT), f32)] + volume_scratch(len(groups)),
        compiler_params=params,
    )(near, far, *tables, weight)


def prep_call(masks, links, field, lagrange, mortar, tables, stiff_weight):
    slots = mortar.shape[0]
    patches = 1 << len(masks)
    return pl.pallas_call(
        functools.partial(prep_kernel, masks),
        out_shape=(
            jax.ShapeDtypeStruct((patches, PAD, WIN), f32),
            jax.ShapeDtypeStruct((PAD, WIDE), f32),
            jax.ShapeDtypeStruct((2 * slots, 2, PAD, PAD), f32),
            jax.ShapeDtypeStruct((1, WIN), jnp.int32),
            *(jax.ShapeDtypeStruct(t.shape, bf16) for t in tables),
            jax.ShapeDtypeStruct((QUAD, halfspan), f32),
        ),
        in_specs=[anywhere()] * 10,
        out_specs=(vmem(),) * 10,
        scratch_shapes=[
            pltpu.SMEM(links.shape, jnp.int32),
            pltpu.VMEM(links.shape, jnp.int32),
            pltpu.VMEM(field.shape, f32),
            pltpu.VMEM(lagrange.shape, f32),
            pltpu.VMEM(mortar.shape, f32),
            pltpu.VMEM((PAD, FLAT), f32),
            pltpu.VMEM((8, FLAT), f32),
            pltpu.SemaphoreType.DMA((11,)),
        ],
        compiler_params=params,
    )(*in_hbm(links, field, lagrange, mortar, *tables, stiff_weight))


def final_call(groups, route, sides, kept, other, stiff_a, stiff_b, volume, wides, tables, weight, field):
    slots = sides.shape[0] // 2
    return pl.pallas_call(
        functools.partial(final_kernel, groups),
        out_shape=(
            jax.ShapeDtypeStruct(field.shape, f32),
            jax.ShapeDtypeStruct((slots, 1, 1, BASIS * BASIS), f32),
        ),
        in_specs=[vmem()] * 14,
        out_specs=(vmem(), vmem()),
        scratch_shapes=[pltpu.VMEM((2 * kept.shape[0], PAD, WIN), f32)]
        + volume_scratch(len(groups))
        + [pltpu.SMEM((1, WIN), jnp.int32), pltpu.SemaphoreType.DMA((1,))],
        compiler_params=params,
    )(route, sides, kept, other, stiff_a, stiff_b, volume, wides, *tables, weight)


def swap(array, axis, mask):
    size = lax.axis_size(axis)
    return lax.ppermute(array, axis, [(n, n ^ mask) for n in range(size)])


def after(array, *others):
    return lax.optimization_barrier((array,) + others)[0]


def per_device(state, stiff_weight, volume_weight, lagrange, mortar, links):
    tables = [jnp.asarray(constants()[name]) for name in ("spread", "ahead", "outer", "inner", "back")]
    patches = lax.axis_size("patch")
    masks = [1 << n for n in reversed(range(patches.bit_length() - 1))]
    field = jnp.transpose(state, (0, 1, 3, 2, 4))[0, 0]
    mortar = jnp.transpose(mortar, (0, 1, 3, 2, 4))
    links = links.T

    near = swap(field, "sub", 1)
    own, wide, sides, route, *tables, weight_a = prep_call(masks, links, field, lagrange, mortar, tables, stiff_weight)
    far = swap(jnp.stack([field, near]), "sub", 2)
    first = GROUPS // 2
    stiff_a, weight_b = stiff_call(
        list(range(first)), (halfspan, ELEMS * SPAN - halfspan), wide, tables, weight_a, stiff_weight
    )
    stiff_b, weight_c = stiff_call(list(range(first, GROUPS)), (0, ELEMS * SPAN), wide, tables, weight_b, volume_weight)
    volume, wides = volume_call(list(range(EARLY)), near, far, tables, weight_c)
    gates = [None, stiff_a, stiff_b]
    held = own[None]
    for n, mask in enumerate(masks):
        late = len(masks) - n
        gate = gates[max(0, 3 - late)]
        half = held.shape[1] // 2
        send = held[:, half:]
        other = swap(send if gate is None else after(send, gate), "patch", mask)
        kept = held[:, :half]
        held = jnp.concatenate([kept, other], axis=0)
    residual, constraint = final_call(
        list(range(EARLY, GROUPS)), route, sides, kept[:, 0], other[:, 0], stiff_a, stiff_b, volume, wides, tables, weight_c, field
    )
    return jnp.transpose(residual[None, None], (0, 1, 3, 2, 4)), constraint


def solution(mesh):
    return jax.shard_map(
        per_device,
        mesh=mesh,
        in_specs=(
            P("patch", "sub", None, None, None),
            P("patch", None, None),
            P("patch", None, None),
            P("patch", "sub", None, None),
            P("patch", None, None, None, None),
            P(),
        ),
        out_specs=(P("patch", "sub", None, None, None), P("patch", "sub", None, None)),
        check_vma=False,
    )
```

```python
import functools

import jax
import jax.numpy as jnp
import numpy as np
from jax import lax
from jax.experimental import pallas as pl
from jax.experimental.pallas import tpu as pltpu
from jax.sharding import PartitionSpec as P


ELEMS = 24
DEGREE = 3
FIELDS = 4
LOCAL = DEGREE + 1
NODES = 4
BASIS = ELEMS + DEGREE
QUAD = ELEMS * NODES
PAD = 32
WIN = LOCAL * PAD
SPAN = NODES * QUAD
GROUPS = ELEMS // 4
EARLY = GROUPS - 2
WIDE = (GROUPS + 1) * WIN
FLAT = 768
GROUP_ROWS = 4 * PAD
BLOCK = 256
BLOCK_WIDE = 384

stabilize = 0.25
f32 = jnp.float32
bf16 = jnp.bfloat16
gauss_points_four = [
    -0.8611363115940526,
    -0.3399810435848563,
    0.3399810435848563,
    0.8611363115940526,
]
gauss_weights_four = [
    0.3478548451374538,
    0.6521451548625461,
    0.6521451548625461,
    0.3478548451374538,
]


def spline_tables(knot_list, points, degree):
    current = np.where(
        (knot_list[None, :-1] <= points[:, None]) & (points[:, None] < knot_list[None, 1:]),
        1.0,
        0.0,
    )
    previous = current
    for order_k in range(1, degree + 1):
        previous = current
        amount = len(knot_list) - 1 - order_k
        current = np.zeros((points.shape[0], amount))
        for column in range(amount):
            left_span = knot_list[column + order_k] - knot_list[column]
            right_span = knot_list[column + order_k + 1] - knot_list[column + 1]
            if left_span > 0:
                current[:, column] += (points - knot_list[column]) / left_span * previous[:, column]
            if right_span > 0:
                current[:, column] += (
                    (knot_list[column + order_k + 1] - points)
                    / right_span
                    * previous[:, column + 1]
                )
    slope_part = np.zeros(current.shape)
    for column in range(current.shape[1]):
        left_span = knot_list[column + degree] - knot_list[column]
        right_span = knot_list[column + degree + 1] - knot_list[column + 1]
        if left_span > 0:
            slope_part[:, column] += degree / left_span * previous[:, column]
        if right_span > 0:
            slope_part[:, column] -= degree / right_span * previous[:, column + 1]
    return current, slope_part


def halves(table):
    high = table.astype(np.dtype(bf16)).astype(np.float64)
    return high, table - high


def padded(table, rows, cols):
    out = np.zeros((rows, cols))
    out[: table.shape[0], : table.shape[1]] = table
    return out


@functools.cache
def constants():
    nodes = np.array(gauss_points_four)
    points = (np.arange(ELEMS)[:, None] + (nodes[None, :] + 1.0) / 2.0).reshape(-1)
    weights = np.tile(np.array(gauss_weights_four) / 2.0, ELEMS)
    open_knots = np.concatenate(
        [np.zeros(DEGREE), np.arange(ELEMS + 1.0), np.full(DEGREE, float(ELEMS))]
    )
    even_knots = np.arange(-DEGREE, ELEMS + DEGREE + 1.0)
    value, slope = spline_tables(open_knots, points, DEGREE)
    even_value, even_slope = spline_tables(even_knots, points, DEGREE)
    change = np.round(np.linalg.lstsq(even_value, value, rcond=None)[0] * 4.0) / 4.0
    local_value = even_value[4 * NODES : 5 * NODES, 4 : 4 + LOCAL]
    local_slope = even_slope[4 * NODES : 5 * NODES, 4 : 4 + LOCAL]
    local_w = weights[:NODES, None]

    def kron(local, table):
        wide = padded(table, QUAD, PAD)
        return np.einsum("bj,ck->jkbc", local, wide).reshape(WIN, SPAN)

    ahead = np.concatenate(
        [kron(local_value, value), kron(local_slope, value), kron(local_value, slope)], axis=1
    )
    value_w, slope_w = value * weights[:, None], slope * weights[:, None]
    back = np.concatenate(
        [
            kron(local_value * local_w, value_w).T,
            kron(local_slope * local_w, value_w).T,
            kron(local_value * local_w, slope_w).T,
        ],
        axis=0,
    )
    ahead_high, ahead_low = halves(ahead)
    ahead3 = np.concatenate([ahead_high, ahead_high, ahead_low], axis=0)
    back_high, back_low = halves(back)
    back2 = np.concatenate([back_high, back_low], axis=1)

    def left3(table):
        high, low = halves(padded(table, QUAD, PAD))
        return np.concatenate([high, high, low], axis=1)

    def left4(table):
        high, low = halves(padded(table, QUAD, PAD).T)
        return np.concatenate(
            [np.concatenate([high, high], axis=1), np.concatenate([low, low], axis=1)], axis=0
        )

    spread = np.zeros((BASIS, BASIS, WIDE // PAD, PAD))
    for k in range(BASIS):
        spread[:, k, :BASIS, k] = change.T
    spread = padded(spread.reshape(BASIS * BASIS, WIDE), FLAT, WIDE)
    blocks = [
        spread[n * BLOCK : (n + 1) * BLOCK, n * BLOCK : n * BLOCK + BLOCK_WIDE] for n in range(FLAT // BLOCK)
    ]
    assert sum(np.count_nonzero(block) for block in blocks) == np.count_nonzero(spread)
    as16 = lambda a: a.astype(np.dtype(bf16))
    return dict(
        ahead=as16(ahead3),
        back=as16(back2),
        outer=as16(np.stack([left3(slope), left3(value)])),
        inner=as16(np.stack([left4(slope_w), left4(value_w)])),
        spread=as16(np.stack(blocks)),
    )


def split(x):
    high = x.astype(bf16)
    return high, (x - high.astype(f32)).astype(bf16)


def dot(a, b):
    return jnp.dot(a, b, preferred_element_type=f32)


def dot_nt(a, b):
    return lax.dot_general(a, b, (((1,), (1,)), ((), ())), preferred_element_type=f32)


def expand(fields, spread_ref):
    parts = []
    for field in fields:
        parts.extend(split(field))
    rows = jnp.concatenate(parts, axis=0)
    out = None
    for n in range(FLAT // BLOCK):
        piece = dot(rows[:, n * BLOCK : (n + 1) * BLOCK], spread_ref[n])
        left, right = n * BLOCK, WIDE - n * BLOCK - BLOCK_WIDE
        sides = [jnp.zeros((rows.shape[0], width), f32) for width in (left, right)]
        pieces = ([sides[0]] if left else []) + [piece] + ([sides[1]] if right else [])
        piece = jnp.concatenate(pieces, axis=1)
        out = piece if out is None else out + piece
    return halves_sum(out, len(fields))


def contract(wide, spread_ref):
    rows = jnp.concatenate(split(wide), axis=0)
    out = [
        dot_nt(rows[:, n * BLOCK : n * BLOCK + BLOCK_WIDE], spread_ref[n]) for n in range(FLAT // BLOCK)
    ]
    return halves_sum(jnp.concatenate(out, axis=1), 1)[0]


def halves_sum(out, count):
    return [
        out[2 * n * PAD : (2 * n + 1) * PAD] + out[(2 * n + 1) * PAD : (2 * n + 2) * PAD]
        for n in range(count)
    ]


def shifts(wide):
    rolled = [wide] + [pltpu.roll(wide, WIDE - PAD * r, axis=1) for r in range(1, 4)]
    return [split(x) for x in rolled]


def windows(shifted, m):
    rows = []
    for r in range(4):
        high = shifted[r][0][:, m * WIN : (m + 1) * WIN]
        low = shifted[r][1][:, m * WIN : (m + 1) * WIN]
        rows.append(jnp.concatenate([high, low, high], axis=1))
    return jnp.concatenate(rows, axis=0)


def overlap(rows, groups):
    first, count = groups[0], len(groups)
    total = None
    for r in range(4):
        pieces = []
        if first > 0:
            pieces.append(jnp.zeros((PAD, first * WIN), f32))
        pieces.extend(rows[n][r * PAD : (r + 1) * PAD] for n in range(count))
        rest = WIDE // WIN - first - count
        pieces.append(jnp.zeros((PAD, rest * WIN), f32))
        line = jnp.concatenate(pieces, axis=1)
        if r > 0:
            line = pltpu.roll(line, PAD * r, axis=1)
        total = line if total is None else total + line
    return total


def gather_back(heads_ref, n, back):
    high = heads_ref[n * GROUP_ROWS : (n + 1) * GROUP_ROWS, :]
    low = heads_ref[heads_ref.shape[0] // 2 + n * GROUP_ROWS : heads_ref.shape[0] // 2 + (n + 1) * GROUP_ROWS, :]
    out = dot(jnp.concatenate([high, low], axis=0), back)
    out = out[:GROUP_ROWS] + out[GROUP_ROWS:]
    return out[:, :WIN] + out[:, WIN:]


def load_flat(dst, src):
    dst[...] = jnp.zeros(dst.shape, f32)
    for i in range(BASIS):
        dst[i : i + 1, : BASIS * BASIS] = src[i]


def element_pairs(groups, ahead, outers, inners, planes, back, weight_ref, base, mid_h, mid_l, prod, heads, hooks=None):
    count = len(groups)
    pairs = 2 * count
    half = heads.shape[0] // 2
    done = []

    def forward(p):
        scale = [weight_ref[:, base + (2 * p + q) * SPAN : base + (2 * p + q + 1) * SPAN] for q in range(2)]
        column = 0
        for outer, sources in zip(outers, planes):
            pieces = []
            for q in range(2):
                row = (2 * p + q) * PAD
                for source in sources:
                    stack = []
                    for block in source:
                        cols = slice(block * SPAN, (block + 1) * SPAN)
                        stack += [mid_h[row : row + PAD, cols], mid_l[row : row + PAD, cols], mid_h[row : row + PAD, cols]]
                    pieces.append(jnp.concatenate(stack, axis=0))
            out = dot(outer, jnp.concatenate(pieces, axis=1))
            wide = jnp.concatenate([scale[q] for q in range(2) for _ in sources], axis=1)
            high, low = split(out * wide)
            width = 2 * len(sources) * SPAN
            prod[p % 2, :QUAD, column : column + width] = high
            prod[p % 2, QUAD:, column : column + width] = low
            column += width

    def backward(p):
        column = 0
        place = 0
        for inner, sources in zip(inners, planes):
            width = 2 * len(sources) * SPAN
            out = dot(inner, prod[p % 2, :, column : column + width])
            high, low = split(out[:PAD] + out[PAD:])
            for q in range(2):
                row = (2 * p + q) * PAD
                take = slice(q * len(sources) * SPAN, (q + 1) * len(sources) * SPAN)
                put = slice(place, place + len(sources) * SPAN)
                heads[row : row + PAD, put] = high[:, take]
                heads[half + row : half + row + PAD, put] = low[:, take]
            column += width
            place += len(sources) * SPAN

    ahead(0)
    for p in range(pairs + 1):
        if p < pairs:
            forward(p)
            if p % 2 == 0 and p // 2 + 1 < count:
                ahead(p // 2 + 1)
        if hooks and p in hooks:
            hooks[p]()
        if p > 0:
            backward(p - 1)
        if p >= 3 and p % 2 == 1:
            done.append(gather_back(heads, len(done), back))
    while len(done) < count:
        done.append(gather_back(heads, len(done), back))
    return overlap(done, groups)


def start_all(pairs, sems):
    copies = [pltpu.make_async_copy(src, dst, sems.at[n]) for n, (src, dst) in enumerate(pairs)]
    for copy in copies:
        copy.start()
    return copies


def stiff_kernel(groups, fetch_lanes, wide_ref, ahead_ref, outer_ref, inner_ref, back_ref, weight_ref, next_hbm, out_ref, next_ref, mid_h, mid_l, prod, heads, sems):
    copies = start_all([(next_hbm.at[0, :, fetch_lanes], next_ref)], sems)
    shifted = shifts(wide_ref[...])

    def ahead(n):
        high, low = split(dot(windows(shifted, groups[n]), ahead_ref[...]))
        mid_h[n * GROUP_ROWS : (n + 1) * GROUP_ROWS, :] = high
        mid_l[n * GROUP_ROWS : (n + 1) * GROUP_ROWS, :] = low

    out_ref[...] = element_pairs(
        groups,
        ahead,
        (outer_ref[0], outer_ref[1], outer_ref[1]),
        (inner_ref[0], inner_ref[1], inner_ref[1]),
        (((0,),), ((1,),), ((2,),)),
        back_ref[...],
        weight_ref,
        0,
        mid_h,
        mid_l,
        prod,
        heads,
    )
    for copy in copies:
        copy.wait()


def volume_tables(outer_ref, inner_ref, back_ref):
    sub = lax.axis_index("sub")
    is_pressure = sub == FIELDS - 1
    outer = jnp.concatenate([outer_ref[jnp.where(is_pressure, 0, 1)], outer_ref[1]], axis=1)
    inner = inner_ref[jnp.where(sub == 0, 0, 1)]
    kind = jnp.where(is_pressure, 0, sub)
    back = back_ref[pl.ds(pl.multiple_of(kind * SPAN, SPAN), SPAN), :]
    return outer, inner, back


def volume_groups(groups, wides, ahead_ref, tables, weight_ref, mid_h, mid_l, prod, heads, hooks=None):
    shifted = [shifts(wide) for wide in wides]
    outer, inner, back = tables

    def ahead(n):
        at = slice(n * GROUP_ROWS, (n + 1) * GROUP_ROWS)
        m = groups[n]
        high, low = split(dot(windows(shifted[0], m), ahead_ref[:, :SPAN]))
        mid_h[at, :SPAN] = high
        mid_l[at, :SPAN] = low
        both = jnp.concatenate([windows(shifted[1], m), windows(shifted[2], m)], axis=1)
        high, low = split(dot(both, jnp.concatenate([ahead_ref[:, SPAN : 2 * SPAN], ahead_ref[:, 2 * SPAN :]], axis=0)))
        mid_h[at, SPAN:] = high
        mid_l[at, SPAN:] = low

    base = groups[0] * 4 * SPAN
    return element_pairs(
        groups, ahead, (outer,), (inner,), (((0, 1),),), back, weight_ref, base, mid_h, mid_l, prod, heads, hooks
    )


def volume_kernel(groups, near_ref, far_ref, spread_ref, ahead_ref, outer_ref, inner_ref, back_ref, weight_ref, out_ref, wides_ref, flat, mid_h, mid_l, prod, heads):
    sub = lax.axis_index("sub")
    is_pressure = sub == FIELDS - 1
    load_flat(flat.at[0], near_ref)
    load_flat(flat.at[1], far_ref.at[0])
    load_flat(flat.at[2], far_ref.at[1])
    chosen = jnp.where(is_pressure, 2, 2 - sub)
    zero = jnp.zeros((PAD, FLAT), f32)
    fields = [
        flat[chosen],
        jnp.where(is_pressure, flat[1], zero),
        jnp.where(is_pressure, flat[0], zero),
    ]
    wides = expand(fields, spread_ref)
    for n in range(3):
        wides_ref[n] = wides[n]
    tables = volume_tables(outer_ref, inner_ref, back_ref)
    out_ref[...] = volume_groups(groups, wides, ahead_ref, tables, weight_ref, mid_h, mid_l, prod, heads)


def masked(matrix, limit):
    rows = lax.broadcasted_iota(jnp.int32, matrix.shape, 0)
    return jnp.where(rows < limit, matrix, 0.0)


def layers():
    lanes = lax.broadcasted_iota(jnp.int32, (PAD, FLAT), 1)
    group = jnp.floor((lanes.astype(f32) + 0.5) * (1.0 / BASIS)).astype(jnp.int32)
    rows = lax.broadcasted_iota(jnp.int32, (PAD, FLAT), 0)
    inside = lanes - BASIS * group == rows
    return group, rows, jnp.where(inside, 1.0, 0.0).astype(bf16)


def dot_split(a, b, dims):
    a_high, a_low = split(a)
    b_high, b_low = split(b)
    dims = (dims, ((), ()))
    general = functools.partial(lax.dot_general, dimension_numbers=dims, preferred_element_type=f32)
    return general(a_high, b_high) + (general(a_high, b_low) + general(a_low, b_high))


def position(relative, masks):
    total = jnp.int32(0)
    for n, mask in enumerate(masks):
        total = total + jnp.where(jnp.bitwise_and(relative, mask) != 0, jnp.int32(1 << n), jnp.int32(0))
    return total


def routes(links, lines, mine, slots):
    items = 2 * slots
    patch, face = lines[0:2, :], lines[2:4, :]
    hit = jnp.logical_and(patch == mine, jnp.broadcast_to(lines[4:5, :], patch.shape) > 0)
    index = 2 * lax.broadcasted_iota(jnp.int32, patch.shape, 1) + lax.broadcasted_iota(jnp.int32, patch.shape, 0)
    found = [jnp.sum(jnp.where(jnp.logical_and(hit, face == f), index, 0)) for f in range(4)]
    one = lambda flag: jnp.where(flag, jnp.int32(1), jnp.int32(0))
    once = lambda flags: jnp.minimum(functools.reduce(jnp.add, flags, jnp.int32(0)), 1)
    owners = [lax.div(item, items) for item in found]
    faces = []
    for f in range(4):
        mates = [(g, one(owners[g] == owners[f])) for g in range(4) if g != f]
        first = once([mate for g, mate in mates if g < f])
        faces.append((owners[f], first, 2 + once([mate * one(found[g] < found[f]) for g, mate in mates])))
    base = mine * slots
    patch = [links[t % 2, base + t // 2] for t in range(items)]
    alive = [links[4, base + t // 2] > 0 for t in range(items)]
    group = [jnp.where(alive[t], patch[t], -1 - t) for t in range(items)]
    face = [links[2 + t % 2, base + t // 2] for t in range(items)]
    lower = [[] for _ in range(items)]
    earlier = [[] for _ in range(items)]
    for t in range(items):
        for u in range(t):
            same = one(group[u] == group[t])
            below = same * one(face[u] < face[t])
            earlier[t].append(same)
            lower[t].append(below)
            lower[u].append(same - below)
    own = [(patch[t], once(lower[t]), 2 + once(earlier[t])) for t in range(items)]
    return faces, own


def place(block, lane):
    wide = jnp.concatenate([block, jnp.zeros((PAD, WIN - PAD), f32)], axis=1)
    return pltpu.roll(wide, lane * PAD, axis=1)


def prep_kernel(masks, links_hbm, field_hbm, lag_hbm, mortar_hbm, spread_hbm, ahead_hbm, outer_hbm, inner_hbm, back_hbm, weight_hbm, own_ref, wide_ref, sides_ref, route_ref, spread_ref, ahead_ref, outer_ref, inner_ref, back_ref, weight_ref, links, lines, field, lag, mortar, flat, line, sems):
    copies = start_all(
        [
            (field_hbm, field),
            (lag_hbm, lag),
            (links_hbm, links),
            (links_hbm, lines),
            (mortar_hbm, mortar),
            (spread_hbm, spread_ref),
            (ahead_hbm, ahead_ref),
            (outer_hbm, outer_ref),
            (inner_hbm, inner_ref),
            (back_hbm, back_ref),
            (weight_hbm.at[0, :, pl.ds(0, weight_ref.shape[1])], weight_ref),
        ],
        sems,
    )
    slots = lag.shape[0]
    items = 2 * slots
    mine = lax.axis_index("patch")
    own_ref[...] = jnp.zeros(own_ref.shape, f32)
    line[...] = jnp.zeros(line.shape, f32)
    sides_ref[...] = jnp.zeros(sides_ref.shape, f32)
    group, rows, fold = layers()
    same = rows == group
    for copy in copies[:5]:
        copy.wait()
    faces, own = routes(links, lines[...], mine, slots)
    load_flat(flat, field)
    for s in range(slots):
        line[s : s + 1, : BASIS * BASIS] = lag[s, 0]
    spreads = [jnp.where(same, line[s : s + 1, :], 0.0) for s in range(slots)]
    spreads += [
        jnp.where(same, flat[0:1, :], 0.0),
        jnp.where(same, flat[BASIS - 1 : BASIS, :], 0.0),
        jnp.where(group == 0, flat[...], 0.0),
        jnp.where(group == BASIS - 1, flat[...], 0.0),
    ]
    parts = []
    for x in spreads:
        parts.extend(split(x))
    squares = halves_sum(dot_nt(jnp.concatenate(parts, axis=0), fold), 4 + slots)
    base = mine * slots
    for s in range(slots):
        for side in range(2):
            for d in range(2):
                sides_ref[2 * s + side, d, :BASIS, :BASIS] = masked(mortar[s, side, :, d, :], links[4 + d, base + s])
    halfway = [dot_split(sides_ref[t, 0], squares[t // 2], ((0,), (0,))) for t in range(items)]
    copies[5].wait()
    (wide,) = expand([flat[...]], spread_ref)
    wide_ref[...] = wide
    for f in range(4):
        patch, first, second = faces[f]
        row = jnp.bitwise_xor(mine, patch)
        own_ref[row] = own_ref[row] + place(squares[slots + f], first)
    for t in range(items):
        both = dot_split(halfway[t], sides_ref[t, 1], ((1,), (0,)))
        patch, first, second = own[t]
        row = jnp.bitwise_xor(mine, patch)
        own_ref[row] = own_ref[row] + place(both if t % 2 == 0 else -both, second)
    entries = []
    for patch, first, second in faces:
        entries += [position(jnp.bitwise_xor(mine, patch), masks), second]
    for patch, first, second in own:
        entries += [position(jnp.bitwise_xor(mine, patch), masks), first]
    lane = lax.broadcasted_iota(jnp.int32, route_ref.shape, 1)
    table = jnp.zeros(route_ref.shape, jnp.int32)
    for n, entry in enumerate(entries):
        table = jnp.where(lane == n, entry, table)
    route_ref[...] = table
    for copy in copies[6:]:
        copy.wait()


def final_kernel(groups, route_vmem, sides_ref, kept_ref, other_ref, stiff_a, stiff_b, volume_ref, wides_ref, spread_ref, ahead_ref, outer_ref, inner_ref, back_ref, weight_ref, out_ref, jump_ref, buf, mid_h, mid_l, prod, heads, route, sems):
    copies = start_all([(route_vmem, route)], sems)
    items = sides_ref.shape[0]
    slots = items // 2
    half = kept_ref.shape[0]
    buf[:half] = kept_ref[...]
    buf[half:] = other_ref[...]
    group, rows, fold = layers()
    same = rows == group
    squares = []
    halfway = []
    both = []

    def pick(n):
        block = buf[route[0, 2 * n]]
        return pltpu.roll(block, lax.rem(WIN - route[0, 2 * n + 1] * PAD, WIN), axis=1)[:, :PAD]

    def start():
        copies[0].wait()
        halfway.extend(dot_split(sides_ref[t, 0], pick(4 + t), ((1,), (0,))) for t in range(items))
        squares.extend(pick(f) for f in range(4))

    def go_on():
        both.extend(dot_split(halfway[t], sides_ref[t, 1], ((1,), (1,))) for t in range(items))

    def end():
        for s in range(slots):
            squares.append(both[2 * s] - both[2 * s + 1])
        parts = []
        for x in squares:
            parts.extend(split(x))
        lines = halves_sum(dot(jnp.concatenate(parts, axis=0), fold), 4 + slots)
        for s in range(slots):
            row = jnp.sum(jnp.where(same, lines[4 + s], 0.0), axis=0, keepdims=True)
            jump_ref[s, 0] = row[:, : BASIS * BASIS]
        low_row = jnp.sum(jnp.where(same, lines[0], 0.0), axis=0, keepdims=True)
        high_row = jnp.sum(jnp.where(same, lines[1], 0.0), axis=0, keepdims=True)
        both.append(
            jnp.where(rows == 0, low_row, 0.0)
            + jnp.where(rows == BASIS - 1, high_row, 0.0)
            + jnp.where(group == 0, lines[2], 0.0)
            + jnp.where(group == BASIS - 1, lines[3], 0.0)
        )

    tables = volume_tables(outer_ref, inner_ref, back_ref)
    volume = volume_groups(
        groups,
        [wides_ref[n] for n in range(3)],
        ahead_ref,
        tables,
        weight_ref,
        mid_h,
        mid_l,
        prod,
        heads,
        {1: start, 2: go_on, 3: end},
    )
    is_pressure = lax.axis_index("sub") == FIELDS - 1
    factor = jnp.where(is_pressure, -stabilize, 1.0).astype(f32)
    total = factor * (stiff_a[...] + stiff_b[...]) - (volume_ref[...] + volume)
    out = contract(total, spread_ref) + both[-1]
    for i in range(BASIS):
        out_ref[i] = out[i : i + 1, : BASIS * BASIS]


def vmem():
    return pl.BlockSpec(memory_space=pltpu.VMEM)


def anywhere():
    return pl.BlockSpec(memory_space=pltpu.HBM)


def in_hbm(*arrays):
    return [pltpu.with_memory_space_constraint(x, pltpu.HBM) for x in arrays]


params = pltpu.CompilerParams(vmem_limit_bytes=24 << 20)
halfspan = (GROUPS // 2) * 4 * SPAN


def stiff_call(groups, fetch, wide, tables, weight, following):
    count = 4 * len(groups)
    lanes = pl.ds(fetch[0], fetch[1])
    return pl.pallas_call(
        functools.partial(stiff_kernel, groups, lanes),
        out_shape=(
            jax.ShapeDtypeStruct((PAD, WIDE), f32),
            jax.ShapeDtypeStruct((QUAD, fetch[1]), f32),
        ),
        in_specs=[vmem()] * 6 + [anywhere()],
        out_specs=(vmem(), vmem()),
        scratch_shapes=[
            pltpu.VMEM((count * PAD, 3 * SPAN), bf16),
            pltpu.VMEM((count * PAD, 3 * SPAN), bf16),
            pltpu.VMEM((2, 2 * QUAD, 6 * SPAN), bf16),
            pltpu.VMEM((2 * count * PAD, 3 * SPAN), bf16),
            pltpu.SemaphoreType.DMA((1,)),
        ],
        compiler_params=params,
    )(wide, *tables[1:], weight, *in_hbm(following))


def volume_scratch(count):
    return [
        pltpu.VMEM((count * GROUP_ROWS, 2 * SPAN), bf16),
        pltpu.VMEM((count * GROUP_ROWS, 2 * SPAN), bf16),
        pltpu.VMEM((2, 2 * QUAD, 2 * SPAN), bf16),
        pltpu.VMEM((2 * count * GROUP_ROWS, SPAN), bf16),
    ]


def volume_call(groups, near, far, tables, weight):
    return pl.pallas_call(
        functools.partial(volume_kernel, groups),
        out_shape=(jax.ShapeDtypeStruct((PAD, WIDE), f32), jax.ShapeDtypeStruct((3, PAD, WIDE), f32)),
        in_specs=[vmem()] * 8,
        out_specs=(vmem(), vmem()),
        scratch_shapes=[pltpu.VMEM((3, PAD, FLAT), f32)] + volume_scratch(len(groups)),
        compiler_params=params,
    )(near, far, *tables, weight)


def prep_call(masks, links, field, lagrange, mortar, tables, stiff_weight):
    slots = mortar.shape[0]
    patches = 1 << len(masks)
    return pl.pallas_call(
        functools.partial(prep_kernel, masks),
        out_shape=(
            jax.ShapeDtypeStruct((patches, PAD, WIN), f32),
            jax.ShapeDtypeStruct((PAD, WIDE), f32),
            jax.ShapeDtypeStruct((2 * slots, 2, PAD, PAD), f32),
            jax.ShapeDtypeStruct((1, WIN), jnp.int32),
            *(jax.ShapeDtypeStruct(t.shape, bf16) for t in tables),
            jax.ShapeDtypeStruct((QUAD, halfspan), f32),
        ),
        in_specs=[anywhere()] * 10,
        out_specs=(vmem(),) * 10,
        scratch_shapes=[
            pltpu.SMEM(links.shape, jnp.int32),
            pltpu.VMEM(links.shape, jnp.int32),
            pltpu.VMEM(field.shape, f32),
            pltpu.VMEM(lagrange.shape, f32),
            pltpu.VMEM(mortar.shape, f32),
            pltpu.VMEM((PAD, FLAT), f32),
            pltpu.VMEM((8, FLAT), f32),
            pltpu.SemaphoreType.DMA((11,)),
        ],
        compiler_params=params,
    )(*in_hbm(links, field, lagrange, mortar, *tables, stiff_weight))


def final_call(groups, route, sides, kept, other, stiff_a, stiff_b, volume, wides, tables, weight, field):
    slots = sides.shape[0] // 2
    return pl.pallas_call(
        functools.partial(final_kernel, groups),
        out_shape=(
            jax.ShapeDtypeStruct(field.shape, f32),
            jax.ShapeDtypeStruct((slots, 1, 1, BASIS * BASIS), f32),
        ),
        in_specs=[vmem()] * 14,
        out_specs=(vmem(), vmem()),
        scratch_shapes=[pltpu.VMEM((2 * kept.shape[0], PAD, WIN), f32)]
        + volume_scratch(len(groups))
        + [pltpu.SMEM((1, WIN), jnp.int32), pltpu.SemaphoreType.DMA((1,))],
        compiler_params=params,
    )(route, sides, kept, other, stiff_a, stiff_b, volume, wides, *tables, weight)


def swap(array, axis, mask):
    size = lax.axis_size(axis)
    return lax.ppermute(array, axis, [(n, n ^ mask) for n in range(size)])


def after(array, *others):
    return lax.optimization_barrier((array,) + others)[0]


def per_device(state, stiff_weight, volume_weight, lagrange, mortar, links):
    tables = [jnp.asarray(constants()[name]) for name in ("spread", "ahead", "outer", "inner", "back")]
    patches = lax.axis_size("patch")
    masks = [1 << n for n in reversed(range(patches.bit_length() - 1))]
    field = jnp.transpose(state, (0, 1, 3, 2, 4))[0, 0]
    mortar = jnp.transpose(mortar, (0, 1, 3, 2, 4))
    links = links.T

    near = swap(field, "sub", 1)
    own, wide, sides, route, *tables, weight_a = prep_call(masks, links, field, lagrange, mortar, tables, stiff_weight)
    far = swap(jnp.stack([field, near]), "sub", 2)
    first = GROUPS // 2
    stiff_a, weight_b = stiff_call(
        list(range(first)), (halfspan, ELEMS * SPAN - halfspan), wide, tables, weight_a, stiff_weight
    )
    stiff_b, weight_c = stiff_call(list(range(first, GROUPS)), (0, ELEMS * SPAN), wide, tables, weight_b, volume_weight)
    volume, wides = volume_call(list(range(EARLY)), near, far, tables, weight_c)
    gates = [None, stiff_a, stiff_b]
    held = own[None]
    for n, mask in enumerate(masks):
        late = len(masks) - n
        gate = gates[max(0, 3 - late)]
        half = held.shape[1] // 2
        send = held[:, half:]
        other = swap(send if gate is None else after(send, gate), "patch", mask)
        kept = held[:, :half]
        held = jnp.concatenate([kept, other], axis=0)
    residual, constraint = final_call(
        list(range(EARLY, GROUPS)), route, sides, kept[:, 0], other[:, 0], stiff_a, stiff_b, volume, wides, tables, weight_c, field
    )
    return jnp.transpose(residual[None, None], (0, 1, 3, 2, 4)), constraint


def solution(mesh):
    return jax.shard_map(
        per_device,
        mesh=mesh,
        in_specs=(
            P("patch", "sub", None, None, None),
            P("patch", None, None),
            P("patch", None, None),
            P("patch", "sub", None, None),
            P("patch", None, None, None, None),
            P(),
        ),
        out_specs=(P("patch", "sub", None, None, None), P("patch", "sub", None, None)),
        check_vma=False,
    )
```

```python
import functools

import jax
import jax.numpy as jnp
import numpy as np
from jax import lax
from jax.experimental import pallas as pl
from jax.experimental.pallas import tpu as pltpu
from jax.sharding import PartitionSpec as P


ELEMS = 24
DEGREE = 3
FIELDS = 4
LOCAL = DEGREE + 1
NODES = 4
BASIS = ELEMS + DEGREE
QUAD = ELEMS * NODES
PAD = 32
WIN = LOCAL * PAD
SPAN = NODES * QUAD
GROUPS = ELEMS // 4
EARLY = GROUPS - 2
WIDE = (GROUPS + 1) * WIN
FLAT = 768
LAST = (BASIS - 1) * BASIS - (FLAT - WIN)
GROUP_ROWS = 4 * PAD
BLOCK = 256
BLOCK_WIDE = 384

stabilize = 0.25
f32 = jnp.float32
bf16 = jnp.bfloat16
gauss_points_four = [
    -0.8611363115940526,
    -0.3399810435848563,
    0.3399810435848563,
    0.8611363115940526,
]
gauss_weights_four = [
    0.3478548451374538,
    0.6521451548625461,
    0.6521451548625461,
    0.3478548451374538,
]


def spline_tables(knot_list, points, degree):
    current = np.where(
        (knot_list[None, :-1] <= points[:, None]) & (points[:, None] < knot_list[None, 1:]),
        1.0,
        0.0,
    )
    previous = current
    for order_k in range(1, degree + 1):
        previous = current
        amount = len(knot_list) - 1 - order_k
        current = np.zeros((points.shape[0], amount))
        for column in range(amount):
            left_span = knot_list[column + order_k] - knot_list[column]
            right_span = knot_list[column + order_k + 1] - knot_list[column + 1]
            if left_span > 0:
                current[:, column] += (points - knot_list[column]) / left_span * previous[:, column]
            if right_span > 0:
                current[:, column] += (
                    (knot_list[column + order_k + 1] - points)
                    / right_span
                    * previous[:, column + 1]
                )
    slope_part = np.zeros(current.shape)
    for column in range(current.shape[1]):
        left_span = knot_list[column + degree] - knot_list[column]
        right_span = knot_list[column + degree + 1] - knot_list[column + 1]
        if left_span > 0:
            slope_part[:, column] += degree / left_span * previous[:, column]
        if right_span > 0:
            slope_part[:, column] -= degree / right_span * previous[:, column + 1]
    return current, slope_part


def halves(table):
    high = table.astype(np.dtype(bf16)).astype(np.float64)
    return high, table - high


def padded(table, rows, cols):
    out = np.zeros((rows, cols))
    out[: table.shape[0], : table.shape[1]] = table
    return out


@functools.cache
def constants():
    nodes = np.array(gauss_points_four)
    points = (np.arange(ELEMS)[:, None] + (nodes[None, :] + 1.0) / 2.0).reshape(-1)
    weights = np.tile(np.array(gauss_weights_four) / 2.0, ELEMS)
    open_knots = np.concatenate(
        [np.zeros(DEGREE), np.arange(ELEMS + 1.0), np.full(DEGREE, float(ELEMS))]
    )
    even_knots = np.arange(-DEGREE, ELEMS + DEGREE + 1.0)
    value, slope = spline_tables(open_knots, points, DEGREE)
    even_value, even_slope = spline_tables(even_knots, points, DEGREE)
    change = np.round(np.linalg.lstsq(even_value, value, rcond=None)[0] * 4.0) / 4.0
    local_value = even_value[4 * NODES : 5 * NODES, 4 : 4 + LOCAL]
    local_slope = even_slope[4 * NODES : 5 * NODES, 4 : 4 + LOCAL]
    local_w = weights[:NODES, None]

    def kron(local, table):
        wide = padded(table, QUAD, PAD)
        return np.einsum("bj,ck->jkbc", local, wide).reshape(WIN, SPAN)

    ahead = np.concatenate(
        [kron(local_value, value), kron(local_slope, value), kron(local_value, slope)], axis=1
    )
    value_w, slope_w = value * weights[:, None], slope * weights[:, None]
    back = np.concatenate(
        [
            kron(local_value * local_w, value_w).T,
            kron(local_slope * local_w, value_w).T,
            kron(local_value * local_w, slope_w).T,
        ],
        axis=0,
    )
    ahead_high, ahead_low = halves(ahead)
    ahead3 = np.concatenate([ahead_high, ahead_high, ahead_low], axis=0)
    back_high, back_low = halves(back)
    back2 = np.concatenate([back_high, back_low], axis=1)

    def left3(table):
        high, low = halves(padded(table, QUAD, PAD))
        return np.concatenate([high, high, low], axis=1)

    def left4(table):
        high, low = halves(padded(table, QUAD, PAD).T)
        return np.concatenate(
            [np.concatenate([high, high], axis=1), np.concatenate([low, low], axis=1)], axis=0
        )

    spread = np.zeros((BASIS, BASIS, WIDE // PAD, PAD))
    for k in range(BASIS):
        spread[:, k, :BASIS, k] = change.T
    spread = padded(spread.reshape(BASIS * BASIS, WIDE), FLAT, WIDE)
    blocks = [
        spread[n * BLOCK : (n + 1) * BLOCK, n * BLOCK : n * BLOCK + BLOCK_WIDE] for n in range(FLAT // BLOCK)
    ]
    assert sum(np.count_nonzero(block) for block in blocks) == np.count_nonzero(spread)
    as16 = lambda a: a.astype(np.dtype(bf16))
    return dict(
        ahead=as16(ahead3),
        back=as16(back2),
        outer=as16(np.stack([left3(slope), left3(value)])),
        inner=as16(np.stack([left4(slope_w), left4(value_w)])),
        spread=as16(np.stack(blocks)),
    )


def split(x):
    high = x.astype(bf16)
    return high, (x - high.astype(f32)).astype(bf16)


def dot(a, b):
    return jnp.dot(a, b, preferred_element_type=f32)


def dot_nt(a, b):
    return lax.dot_general(a, b, (((1,), (1,)), ((), ())), preferred_element_type=f32)


def expand(fields, spread_ref):
    parts = []
    for field in fields:
        parts.extend(split(field))
    rows = jnp.concatenate(parts, axis=0)
    out = None
    for n in range(FLAT // BLOCK):
        piece = dot(rows[:, n * BLOCK : (n + 1) * BLOCK], spread_ref[n])
        left, right = n * BLOCK, WIDE - n * BLOCK - BLOCK_WIDE
        sides = [jnp.zeros((rows.shape[0], width), f32) for width in (left, right)]
        pieces = ([sides[0]] if left else []) + [piece] + ([sides[1]] if right else [])
        piece = jnp.concatenate(pieces, axis=1)
        out = piece if out is None else out + piece
    return halves_sum(out, len(fields))


def contract(wide, spread_ref):
    rows = jnp.concatenate(split(wide), axis=0)
    out = [
        dot_nt(rows[:, n * BLOCK : n * BLOCK + BLOCK_WIDE], spread_ref[n]) for n in range(FLAT // BLOCK)
    ]
    return halves_sum(jnp.concatenate(out, axis=1), 1)[0]


def halves_sum(out, count):
    return [
        out[2 * n * PAD : (2 * n + 1) * PAD] + out[(2 * n + 1) * PAD : (2 * n + 2) * PAD]
        for n in range(count)
    ]


def shifts(wide):
    rolled = [wide] + [pltpu.roll(wide, WIDE - PAD * r, axis=1) for r in range(1, 4)]
    return [split(x) for x in rolled]


def windows(shifted, m):
    rows = []
    for r in range(4):
        high = shifted[r][0][:, m * WIN : (m + 1) * WIN]
        low = shifted[r][1][:, m * WIN : (m + 1) * WIN]
        rows.append(jnp.concatenate([high, low, high], axis=1))
    return jnp.concatenate(rows, axis=0)


def overlap(rows, groups):
    first, count = groups[0], len(groups)
    total = None
    for r in range(4):
        pieces = []
        if first > 0:
            pieces.append(jnp.zeros((PAD, first * WIN), f32))
        pieces.extend(rows[n][r * PAD : (r + 1) * PAD] for n in range(count))
        rest = WIDE // WIN - first - count
        pieces.append(jnp.zeros((PAD, rest * WIN), f32))
        line = jnp.concatenate(pieces, axis=1)
        if r > 0:
            line = pltpu.roll(line, PAD * r, axis=1)
        total = line if total is None else total + line
    return total


def gather_back(heads_ref, n, back):
    high = heads_ref[n * GROUP_ROWS : (n + 1) * GROUP_ROWS, :]
    low = heads_ref[heads_ref.shape[0] // 2 + n * GROUP_ROWS : heads_ref.shape[0] // 2 + (n + 1) * GROUP_ROWS, :]
    if back.shape[0] == SPAN:
        lower = jnp.concatenate([back[:, :WIN], jnp.zeros((SPAN, WIN), bf16)], axis=1)
        out = dot(jnp.concatenate([high, low], axis=1), jnp.concatenate([back, lower], axis=0))
    else:
        out = dot(jnp.concatenate([high, low], axis=0), back)
        out = out[:GROUP_ROWS] + out[GROUP_ROWS:]
    return out[:, :WIN] + out[:, WIN:]


def load_flat(dst, src):
    dst[...] = jnp.zeros(dst.shape, f32)
    for i in range(BASIS):
        dst[i : i + 1, : BASIS * BASIS] = src[i]


def element_pairs(groups, ahead, outers, inners, planes, back, weight_ref, base, mid_h, mid_l, prod, heads, hooks=None):
    count = len(groups)
    pairs = 2 * count
    half = heads.shape[0] // 2
    done = []

    def forward(p):
        scale = [weight_ref[:, base + (2 * p + q) * SPAN : base + (2 * p + q + 1) * SPAN] for q in range(2)]
        column = 0
        for outer, sources in zip(outers, planes):
            pieces = []
            for q in range(2):
                row = (2 * p + q) * PAD
                for source in sources:
                    stack = []
                    for block in source:
                        cols = slice(block * SPAN, (block + 1) * SPAN)
                        stack += [mid_h[row : row + PAD, cols], mid_l[row : row + PAD, cols], mid_h[row : row + PAD, cols]]
                    pieces.append(jnp.concatenate(stack, axis=0))
            out = dot(outer, jnp.concatenate(pieces, axis=1))
            wide = jnp.concatenate([scale[q] for q in range(2) for _ in sources], axis=1)
            high, low = split(out * wide)
            width = 2 * len(sources) * SPAN
            prod[p % 2, :QUAD, column : column + width] = high
            prod[p % 2, QUAD:, column : column + width] = low
            column += width

    def backward(p):
        column = 0
        place = 0
        for inner, sources in zip(inners, planes):
            width = 2 * len(sources) * SPAN
            out = dot(inner, prod[p % 2, :, column : column + width])
            high, low = split(out[:PAD] + out[PAD:])
            for q in range(2):
                row = (2 * p + q) * PAD
                take = slice(q * len(sources) * SPAN, (q + 1) * len(sources) * SPAN)
                put = slice(place, place + len(sources) * SPAN)
                heads[row : row + PAD, put] = high[:, take]
                heads[half + row : half + row + PAD, put] = low[:, take]
            column += width
            place += len(sources) * SPAN

    ahead(0)
    for p in range(pairs + 1):
        if p < pairs:
            forward(p)
            if p % 2 == 0 and p // 2 + 1 < count:
                ahead(p // 2 + 1)
        if hooks and p in hooks:
            hooks[p]()
        if p > 0:
            backward(p - 1)
        if p >= 3 and p % 2 == 1:
            done.append(gather_back(heads, len(done), back))
    while len(done) < count:
        done.append(gather_back(heads, len(done), back))
    return overlap(done, groups)


def start_all(pairs, sems):
    copies = [pltpu.make_async_copy(src, dst, sems.at[n]) for n, (src, dst) in enumerate(pairs)]
    for copy in copies:
        copy.start()
    return copies


def stiff_kernel(groups, fetch_lanes, wide_ref, ahead_ref, outer_ref, inner_ref, back_ref, weight_ref, next_hbm, out_ref, next_ref, mid_h, mid_l, prod, heads, sems):
    copies = start_all([(next_hbm.at[0, :, fetch_lanes], next_ref)], sems)
    shifted = shifts(wide_ref[...])

    def ahead(n):
        high, low = split(dot(windows(shifted, groups[n]), ahead_ref[...]))
        mid_h[n * GROUP_ROWS : (n + 1) * GROUP_ROWS, :] = high
        mid_l[n * GROUP_ROWS : (n + 1) * GROUP_ROWS, :] = low

    out_ref[...] = element_pairs(
        groups,
        ahead,
        (outer_ref[0], outer_ref[1], outer_ref[1]),
        (inner_ref[0], inner_ref[1], inner_ref[1]),
        (((0,),), ((1,),), ((2,),)),
        back_ref[...],
        weight_ref,
        0,
        mid_h,
        mid_l,
        prod,
        heads,
    )
    for copy in copies:
        copy.wait()


def volume_tables(outer_ref, inner_ref, back_ref):
    sub = lax.axis_index("sub")
    is_pressure = sub == FIELDS - 1
    outer = jnp.concatenate([outer_ref[jnp.where(is_pressure, 0, 1)], outer_ref[1]], axis=1)
    inner = inner_ref[jnp.where(sub == 0, 0, 1)]
    kind = jnp.where(is_pressure, 0, sub)
    back = back_ref[pl.ds(pl.multiple_of(kind * SPAN, SPAN), SPAN), :]
    return outer, inner, back


def volume_groups(groups, wides, ahead_ref, tables, weight_ref, mid_h, mid_l, prod, heads, hooks=None):
    shifted = [shifts(wide) for wide in wides]
    outer, inner, back = tables

    def ahead(n):
        at = slice(n * GROUP_ROWS, (n + 1) * GROUP_ROWS)
        m = groups[n]
        high, low = split(dot(windows(shifted[0], m), ahead_ref[:, :SPAN]))
        mid_h[at, :SPAN] = high
        mid_l[at, :SPAN] = low
        both = jnp.concatenate([windows(shifted[1], m), windows(shifted[2], m)], axis=1)
        high, low = split(dot(both, jnp.concatenate([ahead_ref[:, SPAN : 2 * SPAN], ahead_ref[:, 2 * SPAN :]], axis=0)))
        mid_h[at, SPAN:] = high
        mid_l[at, SPAN:] = low

    base = groups[0] * 4 * SPAN
    return element_pairs(
        groups, ahead, (outer,), (inner,), (((0, 1),),), back, weight_ref, base, mid_h, mid_l, prod, heads, hooks
    )


def volume_kernel(groups, near_ref, far_ref, spread_ref, ahead_ref, outer_ref, inner_ref, back_ref, weight_ref, out_ref, wides_ref, flat, mid_h, mid_l, prod, heads):
    sub = lax.axis_index("sub")
    is_pressure = sub == FIELDS - 1
    load_flat(flat.at[0], near_ref)
    load_flat(flat.at[1], far_ref.at[0])
    load_flat(flat.at[2], far_ref.at[1])
    chosen = jnp.where(is_pressure, 2, 2 - sub)
    zero = jnp.zeros((PAD, FLAT), f32)
    fields = [
        flat[chosen],
        jnp.where(is_pressure, flat[1], zero),
        jnp.where(is_pressure, flat[0], zero),
    ]
    wides = expand(fields, spread_ref)
    for n in range(3):
        wides_ref[n] = wides[n]
    tables = volume_tables(outer_ref, inner_ref, back_ref)
    out_ref[...] = volume_groups(groups, wides, ahead_ref, tables, weight_ref, mid_h, mid_l, prod, heads)


def masked(matrix, limit):
    rows = lax.broadcasted_iota(jnp.int32, matrix.shape, 0)
    return jnp.where(rows < limit, matrix, 0.0)


def layers():
    lanes = lax.broadcasted_iota(jnp.int32, (PAD, FLAT), 1)
    group = jnp.floor((lanes.astype(f32) + 0.5) * (1.0 / BASIS)).astype(jnp.int32)
    rows = lax.broadcasted_iota(jnp.int32, (PAD, FLAT), 0)
    inside = lanes - BASIS * group == rows
    return group, rows, jnp.where(inside, 1.0, 0.0).astype(bf16)


def dot_split(a, b, dims):
    a_high, a_low = split(a)
    b_high, b_low = split(b)
    dims = (dims, ((), ()))
    general = functools.partial(lax.dot_general, dimension_numbers=dims, preferred_element_type=f32)
    return general(a_high, b_high) + (general(a_high, b_low) + general(a_low, b_high))


def position(relative, masks):
    total = jnp.int32(0)
    for n, mask in enumerate(masks):
        total = total + jnp.where(jnp.bitwise_and(relative, mask) != 0, jnp.int32(1 << n), jnp.int32(0))
    return total


def routes(links, lines, mine, slots):
    items = 2 * slots
    patch, face = lines[0:2, :], lines[2:4, :]
    hit = jnp.logical_and(patch == mine, jnp.broadcast_to(lines[4:5, :], patch.shape) > 0)
    index = 2 * lax.broadcasted_iota(jnp.int32, patch.shape, 1) + lax.broadcasted_iota(jnp.int32, patch.shape, 0)
    found = [jnp.sum(jnp.where(jnp.logical_and(hit, face == f), index, 0)) for f in range(4)]
    one = lambda flag: jnp.where(flag, jnp.int32(1), jnp.int32(0))
    once = lambda flags: jnp.minimum(functools.reduce(jnp.add, flags, jnp.int32(0)), 1)
    owners = [lax.div(item, items) for item in found]
    faces = []
    for f in range(4):
        mates = [(g, one(owners[g] == owners[f])) for g in range(4) if g != f]
        first = once([mate for g, mate in mates if g < f])
        faces.append((owners[f], first, 2 + once([mate * one(found[g] < found[f]) for g, mate in mates])))
    base = mine * slots
    patch = [links[t % 2, base + t // 2] for t in range(items)]
    alive = [links[4, base + t // 2] > 0 for t in range(items)]
    group = [jnp.where(alive[t], patch[t], -1 - t) for t in range(items)]
    face = [links[2 + t % 2, base + t // 2] for t in range(items)]
    lower = [[] for _ in range(items)]
    earlier = [[] for _ in range(items)]
    for t in range(items):
        for u in range(t):
            same = one(group[u] == group[t])
            below = same * one(face[u] < face[t])
            earlier[t].append(same)
            lower[t].append(below)
            lower[u].append(same - below)
    own = [(patch[t], once(lower[t]), 2 + once(earlier[t])) for t in range(items)]
    return faces, own


def place(block, lane):
    wide = jnp.concatenate([block, jnp.zeros((PAD, WIN - PAD), f32)], axis=1)
    return pltpu.roll(wide, lane * PAD, axis=1)


def prep_kernel(masks, links_hbm, field_hbm, lag_hbm, mortar_hbm, spread_hbm, ahead_hbm, outer_hbm, inner_hbm, back_hbm, weight_hbm, own_ref, wide_ref, sides_ref, route_ref, spread_ref, ahead_ref, outer_ref, inner_ref, back_ref, weight_ref, links, lines, field, lag, mortar, flat, line, sems):
    copies = start_all(
        [
            (field_hbm, field),
            (lag_hbm, lag),
            (links_hbm, links),
            (links_hbm, lines),
            (mortar_hbm, mortar),
            (spread_hbm, spread_ref),
            (ahead_hbm, ahead_ref),
            (outer_hbm, outer_ref),
            (inner_hbm, inner_ref),
            (back_hbm, back_ref),
            (weight_hbm.at[0, :, pl.ds(0, weight_ref.shape[1])], weight_ref),
        ],
        sems,
    )
    slots = lag.shape[0]
    items = 2 * slots
    mine = lax.axis_index("patch")
    own_ref[...] = jnp.zeros(own_ref.shape, f32)
    line[...] = jnp.zeros(line.shape, f32)
    sides_ref[...] = jnp.zeros(sides_ref.shape, f32)
    group, rows, fold = layers()
    same = rows == group
    for copy in copies[:5]:
        copy.wait()
    faces, own = routes(links, lines[...], mine, slots)
    load_flat(flat, field)
    for s in range(slots):
        line[s : s + 1, : BASIS * BASIS] = lag[s, 0]
    spreads = [jnp.where(same, line[s : s + 1, :], 0.0) for s in range(slots)]
    spreads += [jnp.where(same, flat[0:1, :], 0.0), jnp.where(same, flat[BASIS - 1 : BASIS, :], 0.0)]
    parts = []
    for x in spreads:
        parts.extend(split(x))
    squares = dot_nt(jnp.concatenate(parts, axis=0), fold)
    copies[5].wait()
    (wide,) = expand([flat[...]], spread_ref)
    wide_ref[...] = wide
    squares = halves_sum(squares, 2 + slots)
    inside = lax.broadcasted_iota(jnp.int32, (PAD, PAD), 1) < BASIS
    last = pltpu.roll(flat[:, FLAT - WIN :], WIN - LAST, axis=1)
    squares += [jnp.where(inside, flat[:, :PAD], 0.0), jnp.where(inside, last[:, :PAD], 0.0)]
    base = mine * slots
    for s in range(slots):
        for side in range(2):
            for d in range(2):
                sides_ref[2 * s + side, d, :BASIS, :BASIS] = masked(mortar[s, side, :, d, :], links[4 + d, base + s])
    halfway = [dot_split(sides_ref[t, 0], squares[t // 2], ((0,), (0,))) for t in range(items)]
    for f in range(4):
        patch, first, second = faces[f]
        row = jnp.bitwise_xor(mine, patch)
        own_ref[row] = own_ref[row] + place(squares[slots + f], first)
    for t in range(items):
        both = dot_split(halfway[t], sides_ref[t, 1], ((1,), (0,)))
        patch, first, second = own[t]
        row = jnp.bitwise_xor(mine, patch)
        own_ref[row] = own_ref[row] + place(both if t % 2 == 0 else -both, second)
    entries = []
    for patch, first, second in faces:
        entries += [position(jnp.bitwise_xor(mine, patch), masks), second]
    for patch, first, second in own:
        entries += [position(jnp.bitwise_xor(mine, patch), masks), first]
    lane = lax.broadcasted_iota(jnp.int32, route_ref.shape, 1)
    table = jnp.zeros(route_ref.shape, jnp.int32)
    for n, entry in enumerate(entries):
        table = jnp.where(lane == n, entry, table)
    route_ref[...] = table
    for copy in copies[6:]:
        copy.wait()


def final_kernel(groups, route_vmem, sides_ref, kept_ref, other_ref, stiff_a, stiff_b, volume_ref, wides_ref, spread_ref, ahead_ref, outer_ref, inner_ref, back_ref, weight_ref, out_ref, jump_ref, buf, mid_h, mid_l, prod, heads, route, sems):
    copies = start_all([(route_vmem, route)], sems)
    items = sides_ref.shape[0]
    slots = items // 2
    half = kept_ref.shape[0]
    buf[:half] = kept_ref[...]
    buf[half:] = other_ref[...]
    group, rows, fold = layers()
    same = rows == group
    squares = []
    halfway = []
    both = []

    def pick(n):
        block = buf[route[0, 2 * n]]
        return pltpu.roll(block, lax.rem(WIN - route[0, 2 * n + 1] * PAD, WIN), axis=1)[:, :PAD]

    def start():
        copies[0].wait()
        halfway.extend(dot_split(sides_ref[t, 0], pick(4 + t), ((1,), (0,))) for t in range(items))
        squares.extend(pick(f) for f in range(4))

    def go_on():
        both.extend(dot_split(halfway[t], sides_ref[t, 1], ((1,), (1,))) for t in range(items))

    def end():
        parts = []
        for x in squares[:2] + [both[2 * s] - both[2 * s + 1] for s in range(slots)]:
            parts.extend(split(x))
        lines = halves_sum(dot(jnp.concatenate(parts, axis=0), fold), 2 + slots)
        for s in range(slots):
            row = jnp.sum(jnp.where(same, lines[2 + s], 0.0), axis=0, keepdims=True)
            jump_ref[s, 0] = row[:, : BASIS * BASIS]
        low_row = jnp.sum(jnp.where(same, lines[0], 0.0), axis=0, keepdims=True)
        high_row = jnp.sum(jnp.where(same, lines[1], 0.0), axis=0, keepdims=True)
        low_layer = jnp.concatenate([squares[2], jnp.zeros((PAD, FLAT - PAD), f32)], axis=1)
        high_layer = jnp.concatenate([squares[3], jnp.zeros((PAD, WIN - PAD), f32)], axis=1)
        high_layer = jnp.concatenate(
            [jnp.zeros((PAD, FLAT - WIN), f32), pltpu.roll(high_layer, LAST, axis=1)], axis=1
        )
        both.append(
            jnp.where(rows == 0, low_row, 0.0)
            + jnp.where(rows == BASIS - 1, high_row, 0.0)
            + (low_layer + high_layer)
        )

    tables = volume_tables(outer_ref, inner_ref, back_ref)
    volume = volume_groups(
        groups,
        [wides_ref[n] for n in range(3)],
        ahead_ref,
        tables,
        weight_ref,
        mid_h,
        mid_l,
        prod,
        heads,
        {1: start, 2: go_on, 3: end},
    )
    is_pressure = lax.axis_index("sub") == FIELDS - 1
    factor = jnp.where(is_pressure, -stabilize, 1.0).astype(f32)
    total = factor * (stiff_a[...] + stiff_b[...]) - (volume_ref[...] + volume)
    out = contract(total, spread_ref) + both[-1]
    for i in range(BASIS):
        out_ref[i] = out[i : i + 1, : BASIS * BASIS]


def vmem():
    return pl.BlockSpec(memory_space=pltpu.VMEM)


def anywhere():
    return pl.BlockSpec(memory_space=pltpu.HBM)


def in_hbm(*arrays):
    return [pltpu.with_memory_space_constraint(x, pltpu.HBM) for x in arrays]


params = pltpu.CompilerParams(vmem_limit_bytes=24 << 20)
halfspan = (GROUPS // 2) * 4 * SPAN


def stiff_call(groups, fetch, wide, tables, weight, following):
    count = 4 * len(groups)
    lanes = pl.ds(fetch[0], fetch[1])
    return pl.pallas_call(
        functools.partial(stiff_kernel, groups, lanes),
        out_shape=(
            jax.ShapeDtypeStruct((PAD, WIDE), f32),
            jax.ShapeDtypeStruct((QUAD, fetch[1]), f32),
        ),
        in_specs=[vmem()] * 6 + [anywhere()],
        out_specs=(vmem(), vmem()),
        scratch_shapes=[
            pltpu.VMEM((count * PAD, 3 * SPAN), bf16),
            pltpu.VMEM((count * PAD, 3 * SPAN), bf16),
            pltpu.VMEM((2, 2 * QUAD, 6 * SPAN), bf16),
            pltpu.VMEM((2 * count * PAD, 3 * SPAN), bf16),
            pltpu.SemaphoreType.DMA((1,)),
        ],
        compiler_params=params,
    )(wide, *tables[1:], weight, *in_hbm(following))


def volume_scratch(count):
    return [
        pltpu.VMEM((count * GROUP_ROWS, 2 * SPAN), bf16),
        pltpu.VMEM((count * GROUP_ROWS, 2 * SPAN), bf16),
        pltpu.VMEM((2, 2 * QUAD, 2 * SPAN), bf16),
        pltpu.VMEM((2 * count * GROUP_ROWS, SPAN), bf16),
    ]


def volume_call(groups, near, far, tables, weight):
    return pl.pallas_call(
        functools.partial(volume_kernel, groups),
        out_shape=(jax.ShapeDtypeStruct((PAD, WIDE), f32), jax.ShapeDtypeStruct((3, PAD, WIDE), f32)),
        in_specs=[vmem()] * 8,
        out_specs=(vmem(), vmem()),
        scratch_shapes=[pltpu.VMEM((3, PAD, FLAT), f32)] + volume_scratch(len(groups)),
        compiler_params=params,
    )(near, far, *tables, weight)


def prep_call(masks, links, field, lagrange, mortar, tables, stiff_weight):
    slots = mortar.shape[0]
    patches = 1 << len(masks)
    return pl.pallas_call(
        functools.partial(prep_kernel, masks),
        out_shape=(
            jax.ShapeDtypeStruct((patches, PAD, WIN), f32),
            jax.ShapeDtypeStruct((PAD, WIDE), f32),
            jax.ShapeDtypeStruct((2 * slots, 2, PAD, PAD), f32),
            jax.ShapeDtypeStruct((1, WIN), jnp.int32),
            *(jax.ShapeDtypeStruct(t.shape, bf16) for t in tables),
            jax.ShapeDtypeStruct((QUAD, halfspan), f32),
        ),
        in_specs=[anywhere()] * 10,
        out_specs=(vmem(),) * 10,
        scratch_shapes=[
            pltpu.SMEM(links.shape, jnp.int32),
            pltpu.VMEM(links.shape, jnp.int32),
            pltpu.VMEM(field.shape, f32),
            pltpu.VMEM(lagrange.shape, f32),
            pltpu.VMEM(mortar.shape, f32),
            pltpu.VMEM((PAD, FLAT), f32),
            pltpu.VMEM((8, FLAT), f32),
            pltpu.SemaphoreType.DMA((11,)),
        ],
        compiler_params=params,
    )(*in_hbm(links, field, lagrange, mortar, *tables, stiff_weight))


def final_call(groups, route, sides, kept, other, stiff_a, stiff_b, volume, wides, tables, weight, field):
    slots = sides.shape[0] // 2
    return pl.pallas_call(
        functools.partial(final_kernel, groups),
        out_shape=(
            jax.ShapeDtypeStruct(field.shape, f32),
            jax.ShapeDtypeStruct((slots, 1, 1, BASIS * BASIS), f32),
        ),
        in_specs=[vmem()] * 14,
        out_specs=(vmem(), vmem()),
        scratch_shapes=[pltpu.VMEM((2 * kept.shape[0], PAD, WIN), f32)]
        + volume_scratch(len(groups))
        + [pltpu.SMEM((1, WIN), jnp.int32), pltpu.SemaphoreType.DMA((1,))],
        compiler_params=params,
    )(route, sides, kept, other, stiff_a, stiff_b, volume, wides, *tables, weight)


def swap(array, axis, mask):
    size = lax.axis_size(axis)
    return lax.ppermute(array, axis, [(n, n ^ mask) for n in range(size)])


def after(array, *others):
    return lax.optimization_barrier((array,) + others)[0]


def per_device(state, stiff_weight, volume_weight, lagrange, mortar, links):
    tables = [jnp.asarray(constants()[name]) for name in ("spread", "ahead", "outer", "inner", "back")]
    patches = lax.axis_size("patch")
    masks = [1 << n for n in reversed(range(patches.bit_length() - 1))]
    field = jnp.transpose(state, (0, 1, 3, 2, 4))[0, 0]
    mortar = jnp.transpose(mortar, (0, 1, 3, 2, 4))
    links = links.T

    near = swap(field, "sub", 1)
    own, wide, sides, route, *tables, weight_a = prep_call(masks, links, field, lagrange, mortar, tables, stiff_weight)
    far = swap(jnp.stack([field, near]), "sub", 2)
    first = GROUPS // 2
    stiff_a, weight_b = stiff_call(
        list(range(first)), (halfspan, ELEMS * SPAN - halfspan), wide, tables, weight_a, stiff_weight
    )
    stiff_b, weight_c = stiff_call(list(range(first, GROUPS)), (0, ELEMS * SPAN), wide, tables, weight_b, volume_weight)
    volume, wides = volume_call(list(range(EARLY)), near, far, tables, weight_c)
    gates = [None, stiff_a, stiff_b]
    held = own[None]
    for n, mask in enumerate(masks):
        late = len(masks) - n
        gate = gates[max(0, 3 - late)]
        half = held.shape[1] // 2
        send = held[:, half:]
        other = swap(send if gate is None else after(send, gate), "patch", mask)
        kept = held[:, :half]
        held = jnp.concatenate([kept, other], axis=0)
    residual, constraint = final_call(
        list(range(EARLY, GROUPS)), route, sides, kept[:, 0], other[:, 0], stiff_a, stiff_b, volume, wides, tables, weight_c, field
    )
    return jnp.transpose(residual[None, None], (0, 1, 3, 2, 4)), constraint


def solution(mesh):
    return jax.shard_map(
        per_device,
        mesh=mesh,
        in_specs=(
            P("patch", "sub", None, None, None),
            P("patch", None, None),
            P("patch", None, None),
            P("patch", "sub", None, None),
            P("patch", None, None, None, None),
            P(),
        ),
        out_specs=(P("patch", "sub", None, None, None), P("patch", "sub", None, None)),
        check_vma=False,
    )
```
